32 devices in a mesh: dp: 4 (over z), ctx: 2 (over y), tp: 4 (over x, core).
Axes of the slice: x: 2, y: 2, z: 4, core: 2. Of those that a mesh axis runs over, the one named last changes fastest.
Arguments:
- queries: bfloat16 [1536, 4096], P(('dp', 'ctx'), 'tp'), parts along dimension 0, may hold values from -40 to 40
- keys: bfloat16 [1536, 512], P(('dp', 'ctx'), 'tp'), parts along dimension 0, may hold values from -4 to 4
- values: bfloat16 [1536, 512], P(('dp', 'ctx'), 'tp'), parts along dimension 0, may hold values from -6 to 6
- grad_out: bfloat16 [1536, 4096], P(('dp', 'ctx'), 'tp'), parts along dimension 0, may hold values from -6 to 6
- segments: int32 [1536], P(('dp', 'ctx')), parts along dimension 0, may hold values from 0 to 5, never falling along the last dimension, each value on 1 to 288 neighbouring positions
- sinks: float32 [64], P('tp'), may hold values from -1 to 5
Outputs:
- grad_queries: bfloat16 [1536, 4096], P(('dp', 'ctx'), 'tp'), parts along dimension 0
- keys_gradient: bfloat16 [1536, 512], P(('dp', 'ctx'), 'tp'), parts along dimension 0
- values_gradient: bfloat16 [1536, 512], P(('dp', 'ctx'), 'tp'), parts along dimension 0
- grad_sinks: float32 [256], P(('dp', 'tp')), parts along dimension 0
The draws below stay inside these ranges and needn't reach their ends.
There are 4 independent parts, one for each index of `dp`. The reference program is written for one: setup_inputs(seed, part) draws one part's arguments, and reference() takes and returns one part's arrays. A program takes and returns all parts, laid end to end along the dimension named above; an argument that names none is the same for every part. Nothing has to cross between parts.
All inputs are finite; a program needn't handle non-finite values.
Results may differ from the reference program's by a relative error of at most 0.012.
The reference program's roundings to bfloat16 on the way (of `prob_half` and `dscore`) count: a program that leaves them out, or rounds other values in their place, can miss the bound.
Values may be sent and summed in bfloat16 or wider, within the bound.
No kernel may reach another device: no remote copies, remote signals or barrier semaphores. Data moves between devices by JAX's collectives and lax.ppermute only.
A program may use at most 64 MiB of HBM per device.

```python
import math
import jax
import jax.numpy as jnp
import numpy as np
from jax import lax

QUERY_HEAD_COUNT = 64
KEY_VALUE_HEADS = 8
HEAD_SIZE = 64
DOCS = 6
SEQUENCE_TOKENS = 384


def draw_keys(key, part):
    drawn_result = jax.random.truncated_normal(jax.random.fold_in(key, 11), -4.0, 4.0, (SEQUENCE_TOKENS, KEY_VALUE_HEADS * HEAD_SIZE)).astype(jnp.float32)
    return drawn_result.astype(jnp.bfloat16)


def draw_queries(key, part):
    drawn_result = jax.random.truncated_normal(jax.random.fold_in(key, 12), -4.0, 4.0, (SEQUENCE_TOKENS, QUERY_HEAD_COUNT * HEAD_SIZE)).astype(jnp.float32)
    return drawn_result.astype(jnp.bfloat16)


def block_levels(rng, extent, pieces, least, largest):
    factor_of = 1.0
    for dim, parts in pieces:
        draws = jax.random.uniform(jax.random.fold_in(jax.random.fold_in(rng, 6), dim), (parts,), jnp.float32, least / len(pieces), largest / len(pieces))
        factor_of = factor_of * jnp.repeat(jnp.exp(draws), extent[dim] // parts).reshape((-1,) + (1,) * (len(extent) - 1 - dim))
    return factor_of


def length_profile(count, total, limit, lean):
    portions = [(1 << 20) // math.isqrt(rank ** lean) + 1 for rank in range(2, count + 1)]
    surplus, holding = total - limit - (count - 1), [1] * (count - 1)
    while surplus > 0:
        movable = [i for i in range(count - 1) if holding[i] < limit]
        pool, budget = sum([portions[i] for i in movable]), surplus
        for i in movable:
            addition = min(limit - holding[i], max(1, budget * portions[i] // pool), surplus)
            holding[i] = holding[i] + addition
            surplus = surplus - addition
    return np.array([limit] + holding)


def uneven(key, count, total, most, skew):
    if count == 2:
        one = jax.random.randint(key, (), max(1, total - most), min(most, total - 1) + 1)
        return jnp.stack([one, total - one])
    tallies = jnp.asarray(length_profile(count, total, most, skew), jnp.int32)
    twos = (count - 1) // 2
    donor, taker = tallies[1:1 + 2 * twos:2], tallies[2:2 + 2 * twos:2]
    slack = jnp.minimum(donor - 1, most - taker)
    passed = jax.random.randint(jax.random.fold_in(key, 1), (twos,), 0, 1 << 20) % (slack + 1)
    tallies = tallies.at[1:1 + 2 * twos:2].set(donor - passed).at[2:2 + 2 * twos:2].set(taker + passed)
    return tallies[jax.random.permutation(jax.random.fold_in(key, 2), count)]


def centred(stream_key, dims, width, reach, cuts=(), held_as=jnp.bfloat16):
    result = jax.random.normal(stream_key, dims, jnp.float32) * width
    if len(cuts) > 0:
        result = block_levels(stream_key, dims, cuts, -0.22, 0.18) * result
    return jnp.clip(result, min=-reach, max=reach).astype(held_as)


def setup_inputs(seed: int = 0, part: int = 0) -> dict:
    streams_of = jax.random.split(jax.random.key(seed), 7)
    own_keys = jax.random.split(jax.random.fold_in(streams_of[6], part), 7)
    queries = draw_queries(jax.random.fold_in(jax.random.fold_in(streams_of[6], part), 71), part)
    keys = draw_keys(jax.random.fold_in(jax.random.fold_in(streams_of[6], part), 71), part)
    values = centred(own_keys[2], (SEQUENCE_TOKENS, KEY_VALUE_HEADS * HEAD_SIZE), 1.0, 6.0, ((0, 2), (1, 4)))
    grad_out = centred(own_keys[3], (SEQUENCE_TOKENS, QUERY_HEAD_COUNT * HEAD_SIZE), 1.0, 6.0, ((0, 2), (1, 4)))
    segments = jnp.searchsorted(jnp.cumsum(uneven(own_keys[4], DOCS, SEQUENCE_TOKENS, 3 * SEQUENCE_TOKENS // 4, 0)), jnp.arange(SEQUENCE_TOKENS), side="right").astype(jnp.int32)
    sinks = jnp.clip(-1.0 + 6.0 * jax.random.uniform(streams_of[5], (QUERY_HEAD_COUNT,), jnp.float32) ** block_levels(streams_of[5], (QUERY_HEAD_COUNT,), ((0, 4),), -0.2, 0.2), -1.0, 5.0)
    return {"queries": queries, "keys": keys, "values": values, "grad_out": grad_out, "segments": segments, "sinks": sinks}


def reference(queries, keys, values, grad_out, segments, sinks):
    total_sum = queries.shape[0]
    query_group = QUERY_HEAD_COUNT // KEY_VALUE_HEADS
    scale = HEAD_SIZE ** -0.5
    position = jnp.arange(total_sum, dtype=jnp.int32)
    allowed = (position[None, :] <= position[:, None]) & (segments[None, :] == segments[:, None])

    def one_head(head):
        kv_index = head // query_group
        sink = sinks[head]
        query_head = lax.dynamic_slice_in_dim(queries, (head * HEAD_SIZE).astype(jnp.int32), HEAD_SIZE, 1)
        key_head = lax.dynamic_slice_in_dim(keys, (kv_index * HEAD_SIZE).astype(jnp.int32), HEAD_SIZE, 1)
        value_head = lax.dynamic_slice_in_dim(values, (kv_index * HEAD_SIZE).astype(jnp.int32), HEAD_SIZE, 1)
        grad_head = lax.dynamic_slice_in_dim(grad_out, (head * HEAD_SIZE).astype(jnp.int32), HEAD_SIZE, 1)
        raw = jnp.dot(query_head, key_head.T, preferred_element_type=jnp.float32) * scale
        masked = jnp.where(allowed, raw, -jnp.inf)
        top = jnp.maximum(jnp.max(masked, axis=1), sink)
        lse = top + jnp.log(jnp.exp(sink - top) + jnp.sum(jnp.exp(masked - top[:, None]), axis=1))
        prob = jnp.where(allowed, jnp.exp(raw - lse[:, None]), jnp.float32(0.0))
        prob_half = prob.astype(jnp.bfloat16)
        out = jnp.dot(prob_half, value_head, preferred_element_type=jnp.float32)
        delta = jnp.sum(grad_head.astype(jnp.float32) * out, axis=1)
        grad_sink = -jnp.sum(jnp.exp(sink - lse) * delta)
        dprob = jnp.dot(grad_head, value_head.T, preferred_element_type=jnp.float32)
        dscore = (prob * (dprob - delta[:, None])).astype(jnp.bfloat16)
        grad_query = jnp.dot(dscore, key_head, preferred_element_type=jnp.float32) * scale
        key_gradient = jnp.dot(dscore.T, query_head, preferred_element_type=jnp.float32) * scale
        value_gradient = jnp.dot(prob_half.T, grad_head, preferred_element_type=jnp.float32)
        return grad_query, key_gradient, value_gradient, grad_sink

    grad_query, key_gradient, value_gradient, grad_sinks = lax.map(one_head, jnp.arange(QUERY_HEAD_COUNT, dtype=jnp.int32))
    grad_queries = grad_query.transpose(1, 0, 2).reshape(total_sum, QUERY_HEAD_COUNT * HEAD_SIZE).astype(jnp.bfloat16)
    keys_gradient = key_gradient.reshape(KEY_VALUE_HEADS, query_group, total_sum, HEAD_SIZE).sum(axis=1)
    values_gradient = value_gradient.reshape(KEY_VALUE_HEADS, query_group, total_sum, HEAD_SIZE).sum(axis=1)
    keys_gradient = keys_gradient.transpose(1, 0, 2).reshape(total_sum, KEY_VALUE_HEADS * HEAD_SIZE).astype(jnp.bfloat16)
    values_gradient = values_gradient.transpose(1, 0, 2).reshape(total_sum, KEY_VALUE_HEADS * HEAD_SIZE).astype(jnp.bfloat16)
    return grad_queries, keys_gradient, values_gradient, grad_sinks
```

```python
import functools

import jax
import jax.numpy as jnp
from jax import lax
from jax.experimental import pallas as pl
from jax.experimental.pallas import tpu as pltpu
from jax.sharding import PartitionSpec as P

HEAD_SIZE = 64
LANES = 128
BLOCK = 64
NEG = -1e30
F32 = jnp.float32
BF16 = jnp.bfloat16


def dot(left, right, left_dim, right_dim):
    return lax.dot_general(
        left, right, (((left_dim,), (right_dim,)), ((), ())), preferred_element_type=F32
    )


def over_tiles(count, body, carry):
    if count == 1:
        return body(0, carry)
    return lax.fori_loop(0, count, body, carry)


class Keep:
    def __init__(self, ref, count):
        self.ref, self.inline = ref, count == 1

    def put(self, tile, value):
        if self.inline:
            self.value = value
        else:
            self.ref[tile] = value

    def get(self, tile):
        return self.value if self.inline else self.ref[tile]


def columns(row):
    return jnp.broadcast_to(row, (LANES, row.shape[1])).T


def split_halves(block):
    lane = lax.broadcasted_iota(jnp.int32, block.shape, 1)
    wide = block.astype(F32)
    turned = pltpu.roll(wide, HEAD_SIZE, 1)
    low = lane < HEAD_SIZE
    zero = jnp.zeros_like(wide)
    first = (jnp.where(low, wide, zero), jnp.where(low, zero, turned))
    second = (jnp.where(low, turned, zero), jnp.where(low, zero, wide))
    return tuple((a.astype(BF16), b.astype(BF16)) for a, b in (first, second))


def seg_features(seg_col, blocked):
    lane = lax.broadcasted_iota(jnp.int32, seg_col.shape, 1)
    other = (lane - BLOCK) != seg_col.astype(jnp.int32)
    if blocked is not None:
        other = other | blocked
    return jnp.where((lane >= BLOCK) & other, NEG, 0.0)


def merge_heads(parts):
    lane = lax.broadcasted_iota(jnp.int32, parts[0][0].shape, 1)
    low = lane < HEAD_SIZE
    (first_low, first_high), (second_low, second_high) = parts
    straight = jnp.where(low, first_low, second_high)
    crossed = jnp.where(low, second_low, first_high)
    return straight + pltpu.roll(crossed, HEAD_SIZE, 1)


def main_kernel(
    remote, ctx_axis, kv_heads, pairs,
    q_ref, k_ref, v_ref, g_ref, seg_ref, sink_ref, far_ref,
    dq_ref, own_ref, part_ref, sinks_out_ref,
    s_keep, dp_keep, p_keep, ds_keep, lhs_keep,
):
    length = q_ref.shape[0]
    blocks = length // BLOCK
    width = pairs * BLOCK
    scale = HEAD_SIZE ** (-0.5)
    place = lax.axis_index(ctx_axis)

    seg_col = columns(seg_ref[...].astype(F32))
    lane = lax.broadcasted_iota(jnp.int32, (length, LANES), 1)
    row = lax.broadcasted_iota(jnp.int32, (length, LANES), 0)
    inner = row % BLOCK
    key_seg = seg_features(seg_col, None)
    key_plain = key_seg.astype(BF16)
    key_diag = jnp.where(lane == inner, 1.0, key_seg).astype(BF16)
    same = (lane - BLOCK) == seg_col.astype(jnp.int32)
    query_feat = jnp.where(
        lane < BLOCK, jnp.where(lane > inner, NEG, 0.0), jnp.where(same, 1.0, 0.0)
    ).astype(BF16)

    lane_row = lax.broadcasted_iota(jnp.int32, (1, width), 1)
    far_feat = Keep(lhs_keep, remote)

    def make_feat(tile, carry):
        far = far_ref[tile]
        rows = far[2 * length :].astype(F32)
        pieces = [columns(rows[i : i + 1]) for i in range(-(-length // LANES))]
        far_col = jnp.concatenate(pieces, axis=0)[:length]
        gone = jnp.full((length, LANES), place - 1 - tile) < 0
        far_feat.put(tile, seg_features(far_col, gone).astype(BF16))
        return carry

    over_tiles(remote, make_feat, 0)

    for first in range(0, kv_heads, 2):
        span = slice(first * HEAD_SIZE, (first + 2) * HEAD_SIZE)
        key_halves = split_halves(k_ref[:, span].astype(F32) * scale)
        value_halves = split_halves(v_ref[:, span])
        key_sums, value_sums, far_key_sums, far_value_sums = [], [], {}, {}
        for local in range(2):
            head = first + local
            keys, values = key_halves[local], value_halves[local]
            p_diag, ds_diag, q_rows, g_rows = [], [], [], []
            far_p = [Keep(p_keep.at[block], remote) for block in range(blocks)]
            far_ds = [Keep(ds_keep.at[block], remote) for block in range(blocks)]

            def far_halves(tile, which, local=local, span=span):
                start = which * length
                block = far_ref[tile, start : start + length, span]
                factor = scale if which == 0 else 1.0
                return split_halves(block.astype(F32) * factor)[local]

            sink_rows = [None, None]
            sink_sums = [0.0, 0.0]
            for half in range(2):
                sink_row = jnp.zeros((1, width), F32)
                for pair in range(pairs):
                    value = sink_ref[head * 2 * pairs + 2 * pair + half]
                    sink_row = jnp.where(lane_row // BLOCK == pair, value, sink_row)
                sink_rows[half] = sink_row

            for block in range(blocks):
                rows = slice(block * BLOCK, (block + 1) * BLOCK)
                count = (block + 1) * BLOCK
                lanes_of = [
                    slice((head * pairs + pair) * LANES, (head * pairs + pair + 1) * LANES)
                    for pair in range(pairs)
                ]
                q_stack = jnp.concatenate([q_ref[rows, at] for at in lanes_of], axis=0)
                g_stack = jnp.concatenate([g_ref[rows, at] for at in lanes_of], axis=0)
                feat = jnp.concatenate([query_feat[rows]] * pairs, axis=0)
                q_wide = jnp.concatenate([q_stack, feat], axis=1)
                q_rows.append(q_stack)
                g_rows.append(g_stack)

                feat_k = key_diag[rows]
                if block:
                    feat_k = jnp.concatenate([key_plain[: count - BLOCK], feat_k], axis=0)
                key_near = jnp.concatenate([keys[0][:count], keys[1][:count]], axis=0)
                key_wide = jnp.concatenate(
                    [key_near, jnp.concatenate([feat_k, feat_k], axis=0)], axis=1
                )
                value_near = jnp.concatenate([values[0][:count], values[1][:count]], axis=0)

                s_near = dot(key_wide, q_wide, 1, 1)
                tops = [
                    jnp.maximum(
                        jnp.max(s_near[half * count : (half + 1) * count], axis=0, keepdims=True),
                        sink_rows[half],
                    )
                    for half in range(2)
                ]
                far_s, far_dp = Keep(s_keep, remote), Keep(dp_keep, remote)

                def halves(array):
                    return array[:length], array[length:]

                def spread(pair_of_rows, size):
                    return jnp.concatenate(
                        [jnp.broadcast_to(r, (size, width)) for r in pair_of_rows], axis=0
                    )

                def score_far(tile, carry):
                    low, high = far_halves(tile, 0)
                    feats = far_feat.get(tile)
                    wide = jnp.concatenate(
                        [
                            jnp.concatenate([low, high], axis=0),
                            jnp.concatenate([feats, feats], axis=0),
                        ],
                        axis=1,
                    )
                    scores = dot(wide, q_wide, 1, 1)
                    far_s.put(tile, scores)
                    return tuple(
                        jnp.maximum(c, jnp.max(part, axis=0, keepdims=True))
                        for c, part in zip(carry, halves(scores))
                    )

                tops = over_tiles(remote, score_far, tuple(tops))
                e_near = jnp.exp(s_near - spread(tops, count))
                sink_mass = [jnp.exp(sink_rows[half] - tops[half]) for half in range(2)]
                mass = tuple(
                    sink_mass[half]
                    + jnp.sum(e_near[half * count : (half + 1) * count], axis=0, keepdims=True)
                    for half in range(2)
                )

                def mass_far(tile, carry):
                    weight = jnp.exp(far_s.get(tile) - spread(tops, length))
                    far_s.put(tile, weight)
                    return tuple(
                        c + jnp.sum(part, axis=0, keepdims=True)
                        for c, part in zip(carry, halves(weight))
                    )

                mass = over_tiles(remote, mass_far, mass)
                inverse = [1.0 / m for m in mass]
                p_near = e_near * spread(inverse, count)
                p_half = p_near.astype(BF16)
                p_diag.append(p_half)
                dp_near = dot(value_near, g_stack, 1, 1)
                prod = p_half.astype(F32) * dp_near
                delta = tuple(
                    jnp.sum(prod[half * count : (half + 1) * count], axis=0, keepdims=True)
                    for half in range(2)
                )

                def delta_far(tile, carry):
                    prob = far_s.get(tile) * spread(inverse, length)
                    far_s.put(tile, prob)
                    rounded = prob.astype(BF16)
                    far_p[block].put(tile, rounded)
                    low, high = far_halves(tile, 1)
                    dprob = dot(jnp.concatenate([low, high], axis=0), g_stack, 1, 1)
                    far_dp.put(tile, dprob)
                    return tuple(
                        c + jnp.sum(part, axis=0, keepdims=True)
                        for c, part in zip(carry, halves(rounded.astype(F32) * dprob))
                    )

                delta = over_tiles(remote, delta_far, delta)
                for half in range(2):
                    sink_sums[half] = (
                        sink_sums[half] - sink_mass[half] * inverse[half] * delta[half]
                    )
                ds_near = (p_near * (dp_near - spread(delta, count))).astype(BF16)
                ds_diag.append(ds_near)
                dq = dot(ds_near, key_near, 0, 0)

                def dscore_far(tile, carry):
                    dscore = far_s.get(tile) * (far_dp.get(tile) - spread(delta, length))
                    dscore = dscore.astype(BF16)
                    far_ds[block].put(tile, dscore)
                    low, high = far_halves(tile, 0)
                    return carry + dot(dscore, jnp.concatenate([low, high], axis=0), 0, 0)

                dq = over_tiles(remote, dscore_far, dq)
                for pair in range(pairs):
                    dq_ref[rows, lanes_of[pair]] = dq[pair * BLOCK : (pair + 1) * BLOCK].astype(
                        BF16
                    )

            for half in range(2):
                sinks_out_ref[2 * head + half : 2 * head + half + 1, :] = sink_sums[half]

            def near_sum(parts, rows_of):
                out = [[], []]
                for kb in range(blocks):
                    left = []
                    for block in range(kb, blocks):
                        count = (block + 1) * BLOCK
                        low = parts[block][kb * BLOCK : (kb + 1) * BLOCK]
                        high = parts[block][count + kb * BLOCK : count + (kb + 1) * BLOCK]
                        left.append(jnp.concatenate([low, high], axis=0))
                    total = dot(
                        jnp.concatenate(left, axis=1), jnp.concatenate(rows_of[kb:], axis=0), 1, 0
                    )
                    out[0].append(total[:BLOCK])
                    out[1].append(total[BLOCK:])
                return tuple(jnp.concatenate(o, axis=0) for o in out)

            value_sums.append(near_sum(p_diag, g_rows))
            key_sums.append(near_sum(ds_diag, q_rows))
            q_all = jnp.concatenate(q_rows, axis=0)
            g_all = jnp.concatenate(g_rows, axis=0)

            def far_sum(tile, carry, local=local):
                for which, parts, right in ((0, far_ds, q_all), (1, far_p, g_all)):
                    left = jnp.concatenate([part.get(tile) for part in parts], axis=1)
                    total = dot(left, right, 1, 0)
                    if remote == 1:
                        (far_key_sums, far_value_sums)[which][local] = halves(total)
                    else:
                        at = slice(which * length, (which + 1) * length)
                        lane = lax.broadcasted_iota(jnp.int32, (length, LANES), 1)
                        low = lane < HEAD_SIZE
                        a, b = halves(total)
                        turned = pltpu.roll(jnp.where(low, a, b), HEAD_SIZE, 1)
                        both = (a if local == 0 else b) + turned
                        keep = low if local == 0 else ~low
                        factor = scale if which == 0 else 1.0
                        old = part_ref[tile, at, span]
                        part_ref[tile, at, span] = jnp.where(
                            keep, (both * factor).astype(BF16), old
                        )
                return carry

            over_tiles(remote, far_sum, 0)

        own_ref[0, :, span] = merge_heads(key_sums) * scale
        own_ref[1, :, span] = merge_heads(value_sums)
        if remote == 1:
            part_ref[0, :length, span] = (merge_heads([far_key_sums[i] for i in range(2)]) * scale).astype(BF16)
            part_ref[0, length : 2 * length, span] = merge_heads(
                [far_value_sums[i] for i in range(2)]
            ).astype(BF16)

    sink_rest = sinks_out_ref[...]
    thirds = []
    for _ in range(3):
        top = sink_rest.astype(BF16)
        thirds.append(top)
        sink_rest = sink_rest - top.astype(F32)
    for tile in range(remote):
        for i, piece in enumerate(thirds):
            for j in range(width // LANES):
                at = 2 * length + 16 * (i * (width // LANES) + j)
                part_ref[tile, at : at + 2 * kv_heads, 0:LANES] = piece[:, j * LANES : (j + 1) * LANES]


def last_kernel(remote, pairs, own_ref, back_ref, sinks_ref, dk_ref, dv_ref, out_ref):
    length = dk_ref.shape[0]
    totals = [own_ref[0], own_ref[1]]
    sink = sinks_ref[...]
    heads2 = sink.shape[0]
    width = sink.shape[1]
    for tile in range(remote):
        for which in range(2):
            at = slice(which * length, (which + 1) * length)
            totals[which] = totals[which] + back_ref[tile, at].astype(F32)
        rest = jnp.zeros_like(sink)
        for i in range(3):
            pieces = []
            for j in range(width // LANES):
                at = 2 * length + 16 * (i * (width // LANES) + j)
                pieces.append(back_ref[tile, at : at + heads2, 0:LANES].astype(F32))
            rest = rest + jnp.concatenate(pieces, axis=1)
        sink = sink + rest
    dk_ref[...] = totals[0].astype(BF16)
    dv_ref[...] = totals[1].astype(BF16)
    lane = lax.broadcasted_iota(jnp.int32, (heads2, width), 1)
    out_lane = lax.broadcasted_iota(jnp.int32, out_ref.shape, 1)
    line = jnp.zeros(out_ref.shape, F32)
    for pair in range(pairs):
        sums = jnp.sum(jnp.where(lane // BLOCK == pair, sink, 0.0), axis=1, keepdims=True)
        for r in range(heads2):
            at = (r // 2) * 2 * pairs + 2 * pair + r % 2
            line = jnp.where(out_lane == at, sums[r : r + 1], line)
    out_ref[...] = line


def on_device(ctx_size, queries, keys, values, grad_out, segments, sinks):
    length = queries.shape[0]
    kv_heads = keys.shape[1] // HEAD_SIZE
    pairs = queries.shape[1] // keys.shape[1] // 2
    width = pairs * BLOCK
    blocks = length // BLOCK
    remote = ctx_size - 1
    cols = keys.shape[1]

    seg_rows = -(-length // LANES)
    seg_line = jnp.pad(segments, (0, seg_rows * LANES - length)).astype(BF16)
    seg_block = jnp.pad(
        seg_line.reshape(seg_rows, LANES), ((0, 16 - seg_rows), (0, cols - LANES))
    )
    packed = jnp.concatenate([keys, values, seg_block], axis=0)

    def turn(array, shift):
        order = [(i, (i + shift) % ctx_size) for i in range(ctx_size)]
        return lax.ppermute(array, "ctx", order)

    far = jnp.stack([turn(packed, s) for s in range(1, ctx_size)])

    extra = 16 * 3 * (width // LANES)
    tall = 2 * length + extra
    vmem = pl.BlockSpec(memory_space=pltpu.VMEM)
    smem = pl.BlockSpec(memory_space=pltpu.SMEM)
    many = remote if remote > 1 else 1
    small = remote == 1

    def scratch(shape, dtype):
        return pltpu.VMEM((8, LANES) if small else shape, dtype)

    dq, own, part, sink_rows = pl.pallas_call(
        functools.partial(main_kernel, remote, "ctx", kv_heads, pairs),
        out_shape=(
            jax.ShapeDtypeStruct(queries.shape, BF16),
            jax.ShapeDtypeStruct((2,) + keys.shape, F32),
            jax.ShapeDtypeStruct((remote, tall, cols), BF16),
            jax.ShapeDtypeStruct((2 * kv_heads, width), F32),
        ),
        in_specs=[vmem, vmem, vmem, vmem, vmem, smem, vmem],
        out_specs=(vmem, vmem, vmem, vmem),
        scratch_shapes=[
            pltpu.VMEM((1, 8, LANES) if small else (many, 2 * length, width), F32),
            pltpu.VMEM((1, 8, LANES) if small else (many, 2 * length, width), F32),
            pltpu.VMEM((blocks, 1, 16, LANES) if small else (blocks, many, 2 * length, width), BF16),
            pltpu.VMEM((blocks, 1, 16, LANES) if small else (blocks, many, 2 * length, width), BF16),
            pltpu.VMEM((1, 16, LANES) if small else (many, length, LANES), BF16),
        ],
    )(queries, keys, values, grad_out, segments.reshape(1, length), sinks, far)

    back = jnp.stack([turn(part[s - 1], -s) for s in range(1, ctx_size)])
    heads = sinks.shape[0]
    dk, dv, line = pl.pallas_call(
        functools.partial(last_kernel, remote, pairs),
        out_shape=(
            jax.ShapeDtypeStruct(keys.shape, BF16),
            jax.ShapeDtypeStruct(values.shape, BF16),
            jax.ShapeDtypeStruct((1, heads), F32),
        ),
        in_specs=[vmem, vmem, vmem],
        out_specs=(vmem, vmem, vmem),
    )(own, back, sink_rows)
    return dq, dk, dv, line.reshape(heads)


def solution(mesh):
    rows = P(("dp", "ctx"), "tp")
    return jax.shard_map(
        functools.partial(on_device, mesh.shape["ctx"]),
        mesh=mesh,
        in_specs=(rows, rows, rows, rows, P(("dp", "ctx")), P("tp")),
        out_specs=(rows, rows, rows, P(("dp", "tp"))),
        check_vma=False,
    )
```

```python
import functools

import jax
import jax.numpy as jnp
from jax import lax
from jax.experimental import pallas as pl
from jax.experimental.pallas import tpu as pltpu
from jax.sharding import PartitionSpec as P

HEAD_SIZE = 64
LANES = 128
BLOCK = 64
NEG = -1e30
F32 = jnp.float32
BF16 = jnp.bfloat16
SCALE = HEAD_SIZE ** (-0.5)


def dot(left, right, left_dim, right_dim):
    return lax.dot_general(
        left, right, (((left_dim,), (right_dim,)), ((), ())), preferred_element_type=F32
    )


def join(parts, axis=0):
    return parts[0] if len(parts) == 1 else jnp.concatenate(parts, axis=axis)


def over_tiles(count, body, carry):
    if count == 1:
        return body(0, carry)
    return lax.fori_loop(0, count, body, carry)


class Keep:
    def __init__(self, ref, count):
        self.ref, self.inline = ref, count == 1

    def put(self, tile, value):
        if self.inline:
            self.value = value
        else:
            self.ref[tile] = value

    def get(self, tile):
        return self.value if self.inline else self.ref[tile]


class Sizes:
    def __init__(self, queries, keys, ctx_size):
        self.length = queries.shape[0]
        self.kv_heads = keys.shape[1] // HEAD_SIZE
        self.pairs = queries.shape[1] // keys.shape[1] // 2
        self.width = self.pairs * BLOCK
        self.blocks = self.length // BLOCK
        self.remote = ctx_size - 1
        self.cols = keys.shape[1]
        self.near = 2 * BLOCK * self.blocks * (self.blocks + 1) // 2
        self.stats = self.kv_heads * self.blocks * 2
        self.seg_rows = -(-self.length // LANES)
        self.slices = self.width // LANES
        self.tall = 2 * self.length + 16 * 3 * self.slices

    def near_at(self, block):
        return slice(BLOCK * block * (block + 1), BLOCK * (block + 1) * (block + 2))

    def stat(self, head, block, half):
        return (head * self.blocks + block) * 2 + half

    def rows(self, block):
        return slice(block * BLOCK, (block + 1) * BLOCK)

    def lanes(self, head, pair):
        at = (head * self.pairs + pair) * LANES
        return slice(at, at + LANES)

    def span(self, head):
        at = head // 2 * LANES
        return slice(at, at + LANES)

    def stack(self, ref, head, block):
        return join([ref[self.rows(block), self.lanes(head, p)] for p in range(self.pairs)])


def columns(row):
    return jnp.broadcast_to(row, (LANES, row.shape[1])).T


def split_halves(block, local):
    lane = lax.broadcasted_iota(jnp.int32, block.shape, 1)
    wide = block.astype(F32)
    turned = pltpu.roll(wide, HEAD_SIZE, 1)
    low = lane < HEAD_SIZE
    zero = jnp.zeros_like(wide)
    if local == 0:
        parts = (jnp.where(low, wide, zero), jnp.where(low, zero, turned))
    else:
        parts = (jnp.where(low, turned, zero), jnp.where(low, zero, wide))
    return [part.astype(BF16) for part in parts]


def seg_features(seg_col, blocked):
    lane = lax.broadcasted_iota(jnp.int32, seg_col.shape, 1)
    other = (lane - BLOCK) != seg_col.astype(jnp.int32)
    if blocked is not None:
        other = other | blocked
    return jnp.where((lane >= BLOCK) & other, NEG, 0.0)


def merge_heads(parts):
    lane = lax.broadcasted_iota(jnp.int32, parts[0][0].shape, 1)
    low = lane < HEAD_SIZE
    (first_low, first_high), (second_low, second_high) = parts
    straight = jnp.where(low, first_low, second_high)
    crossed = jnp.where(low, second_low, first_high)
    return straight + pltpu.roll(crossed, HEAD_SIZE, 1)


def halves(array):
    size = array.shape[0] // 2
    return array[:size], array[size:]


def spread(pair_of_rows, size):
    width = pair_of_rows[0].shape[1]
    return join([jnp.broadcast_to(r, (size, width)) for r in pair_of_rows])


def sink_row(sz, sink_ref, head, half):
    lane = lax.broadcasted_iota(jnp.int32, (1, sz.width), 1)
    line = jnp.zeros((1, sz.width), F32)
    for pair in range(sz.pairs):
        value = sink_ref[head * 2 * sz.pairs + 2 * pair + half]
        line = jnp.where(lane // BLOCK == pair, value, line)
    return line


def pack_kernel(sz, k_ref, v_ref, seg_ref, out_ref, line_ref, k_sem, v_sem, seg_sem):
    seg_copy = pltpu.make_async_copy(seg_ref, line_ref, seg_sem)
    seg_copy.start()
    k_copy = pltpu.make_async_copy(k_ref, out_ref.at[pl.ds(0, sz.length)], k_sem)
    v_copy = pltpu.make_async_copy(v_ref, out_ref.at[pl.ds(sz.length, sz.length)], v_sem)
    k_copy.start()
    v_copy.start()
    seg_copy.wait()
    line = line_ref[...].astype(F32).astype(BF16)
    for i in range(sz.seg_rows):
        count = min(LANES, sz.length - i * LANES)
        at = 2 * sz.length + i
        out_ref[at : at + 1, :count] = line[:, i * LANES : i * LANES + count]
    k_copy.wait()
    v_copy.wait()


def seg_columns(sz, lines):
    lines = lines.astype(F32)
    parts = [columns(lines[i : i + 1, :LANES]) for i in range(sz.seg_rows)]
    return join(parts)[: sz.length]


def near_kernel(
    sz, q_hbm, g_hbm, sink_hbm, own_ref,
    q_ref, g_ref, e_ref, dp_ref, top_ref, mass_ref, feat_ref, sink_rows_ref,
    sink_ref, q_sem, g_sem, sink_sem,
):
    q_copy = pltpu.make_async_copy(q_hbm, q_ref, q_sem)
    g_copy = pltpu.make_async_copy(g_hbm, g_ref, g_sem)
    sink_copy = pltpu.make_async_copy(sink_hbm, sink_ref, sink_sem)
    sink_copy.start()
    q_copy.start()
    g_copy.start()
    shape = (sz.length, LANES)
    length = sz.length
    seg_col = seg_columns(sz, own_ref[2 * length :])
    lane = lax.broadcasted_iota(jnp.int32, shape, 1)
    inner = lax.broadcasted_iota(jnp.int32, shape, 0) % BLOCK
    key_seg = seg_features(seg_col, None)
    key_plain = key_seg.astype(BF16)
    key_diag = jnp.where(lane == inner, 1.0, key_seg).astype(BF16)
    same = (lane - BLOCK) == seg_col.astype(jnp.int32)
    query_feat = jnp.where(
        lane < BLOCK, jnp.where(lane > inner, NEG, 0.0), jnp.where(same, 1.0, 0.0)
    ).astype(BF16)
    feat_ref[...] = query_feat
    sink_copy.wait()
    q_copy.wait()
    g_copy.wait()

    for head in range(sz.kv_heads):
        keys = split_halves(own_ref[:length, sz.span(head)].astype(F32) * SCALE, head % 2)
        values = split_halves(own_ref[length : 2 * length, sz.span(head)], head % 2)
        sinks = [sink_row(sz, sink_ref, head, half) for half in range(2)]
        for half in range(2):
            sink_rows_ref[2 * head + half : 2 * head + half + 1] = sinks[half]
        for block in range(sz.blocks):
            count = (block + 1) * BLOCK
            rows = sz.rows(block)
            q_wide = join(
                [sz.stack(q_ref, head, block), join([query_feat[rows]] * sz.pairs)], 1
            )
            feats = join(([key_plain[: count - BLOCK]] if block else []) + [key_diag[rows]])
            key_wide = join([join([part[:count] for part in keys]), join([feats, feats])], 1)
            scores = dot(key_wide, q_wide, 1, 1)
            tops = [
                jnp.maximum(jnp.max(part, axis=0, keepdims=True), sinks[half])
                for half, part in enumerate(halves(scores))
            ]
            weight = jnp.exp(scores - spread(tops, count))
            at = sz.near_at(block)
            e_ref[head, at] = weight
            for half, part in enumerate(halves(weight)):
                r = sz.stat(head, block, half)
                top_ref[r : r + 1] = tops[half]
                mass_ref[r : r + 1] = jnp.exp(sinks[half] - tops[half]) + jnp.sum(
                    part, axis=0, keepdims=True
                )
            dp_ref[head, at] = dot(
                join([part[:count] for part in values]), sz.stack(g_ref, head, block), 1, 1
            )


def far_kernel(
    sz, ctx_axis, q_ref, g_ref, far_ref, sink_rows_ref, e_ref, dp_ref, top_ref, mass_ref, feat_ref,
    part_ref, ds_ref, ratio_ref, delta_ref, sinks_out_ref,
    s_keep, dp_keep, p_keep, feat_keep,
):
    length, remote = sz.length, sz.remote
    place = lax.axis_index(ctx_axis)
    query_feat = feat_ref[...]
    far_feat = Keep(feat_keep, remote)

    def make_feat(tile, carry):
        far_col = seg_columns(sz, far_ref[tile][2 * length :])
        gone = jnp.full((length, LANES), place - 1 - tile) < 0
        far_feat.put(tile, seg_features(far_col, gone).astype(BF16))
        return carry

    over_tiles(remote, make_feat, 0)
    sums = {}

    for head in range(sz.kv_heads):
        span, local = sz.span(head), head % 2
        q_rows = [sz.stack(q_ref, head, block) for block in range(sz.blocks)]
        g_rows = [sz.stack(g_ref, head, block) for block in range(sz.blocks)]
        sinks = [sink_rows_ref[2 * head + half : 2 * head + half + 1] for half in range(2)]
        sink_sums = [0.0, 0.0]
        far_p = [Keep(p_keep.at[block], remote) for block in range(sz.blocks)]
        far_ds = [Keep(ds_ref.at[head, block], remote) for block in range(sz.blocks)]

        def far_keys(tile):
            return join(split_halves(far_ref[tile, :length, span].astype(F32) * SCALE, local))

        def far_values(tile):
            return join(split_halves(far_ref[tile, length : 2 * length, span], local))

        if remote == 1:
            keys_here, values_here = far_keys(0), far_values(0)
            far_keys, far_values = (lambda tile: keys_here), (lambda tile: values_here)

        for block in range(sz.blocks):
            count = (block + 1) * BLOCK
            q_wide = join([q_rows[block], join([query_feat[sz.rows(block)]] * sz.pairs)], 1)
            g_stack = g_rows[block]
            far_s, far_dp = Keep(s_keep, remote), Keep(dp_keep, remote)
            stat = [sz.stat(head, block, half) for half in range(2)]
            near_tops = [top_ref[r : r + 1] for r in stat]

            def score_far(tile, carry):
                feats = far_feat.get(tile)
                wide = join([far_keys(tile), join([feats, feats])], 1)
                scores = dot(wide, q_wide, 1, 1)
                far_s.put(tile, scores)
                return tuple(
                    jnp.maximum(c, jnp.max(part, axis=0, keepdims=True))
                    for c, part in zip(carry, halves(scores))
                )

            tops = over_tiles(remote, score_far, tuple(near_tops))
            shrink = [jnp.exp(near_tops[half] - tops[half]) for half in range(2)]
            mass = tuple(mass_ref[r : r + 1] * s for r, s in zip(stat, shrink))

            def mass_far(tile, carry):
                weight = jnp.exp(far_s.get(tile) - spread(tops, length))
                far_s.put(tile, weight)
                return tuple(
                    c + jnp.sum(part, axis=0, keepdims=True)
                    for c, part in zip(carry, halves(weight))
                )

            mass = over_tiles(remote, mass_far, mass)
            inverse = [1.0 / m for m in mass]
            ratio = [s * i for s, i in zip(shrink, inverse)]
            at = sz.near_at(block)
            near_half = (e_ref[head, at] * spread(ratio, count)).astype(BF16)
            prod = near_half.astype(F32) * dp_ref[head, at]
            delta = tuple(jnp.sum(part, axis=0, keepdims=True) for part in halves(prod))

            def delta_far(tile, carry):
                prob = far_s.get(tile) * spread(inverse, length)
                far_s.put(tile, prob)
                rounded = prob.astype(BF16)
                far_p[block].put(tile, rounded)
                dprob = dot(far_values(tile), g_stack, 1, 1)
                far_dp.put(tile, dprob)
                return tuple(
                    c + jnp.sum(part, axis=0, keepdims=True)
                    for c, part in zip(carry, halves(rounded.astype(F32) * dprob))
                )

            delta = over_tiles(remote, delta_far, delta)
            for half in range(2):
                sink_prob = jnp.exp(sinks[half] - tops[half]) * inverse[half]
                sink_sums[half] = sink_sums[half] - sink_prob * delta[half]
                ratio_ref[stat[half] : stat[half] + 1] = ratio[half]
                delta_ref[stat[half] : stat[half] + 1] = delta[half]

            def dscore_far(tile, carry):
                dscore = far_s.get(tile) * (far_dp.get(tile) - spread(delta, length))
                dscore = dscore.astype(BF16)
                far_ds[block].put(tile, dscore)
                if remote == 1:
                    ds_ref[head, block, tile] = dscore
                return carry

            over_tiles(remote, dscore_far, 0)

        for half in range(2):
            sinks_out_ref[2 * head + half : 2 * head + half + 1, :] = sink_sums[half]
        q_all, g_all = join(q_rows), join(g_rows)

        def far_sum(tile, carry):
            for which, parts, right in ((0, far_ds, q_all), (1, far_p, g_all)):
                total = dot(join([part.get(tile) for part in parts], 1), right, 1, 0)
                if remote == 1:
                    sums[which, local] = halves(total)
                else:
                    at = slice(which * length, (which + 1) * length)
                    lane = lax.broadcasted_iota(jnp.int32, (length, LANES), 1)
                    low = lane < HEAD_SIZE
                    a, b = halves(total)
                    turned = pltpu.roll(jnp.where(low, a, b), HEAD_SIZE, 1)
                    both = ((a if local == 0 else b) + turned) * (SCALE if which == 0 else 1.0)
                    keep = low if local == 0 else ~low
                    part_ref[tile, at, span] = jnp.where(
                        keep, both.astype(BF16), part_ref[tile, at, span]
                    )
            return carry

        over_tiles(remote, far_sum, 0)
        if remote == 1 and local == 1:
            for which, factor in ((0, SCALE), (1, 1.0)):
                merged = merge_heads([sums[which, 0], sums[which, 1]]) * factor
                part_ref[0, which * length : (which + 1) * length, span] = merged.astype(BF16)

    rest = sinks_out_ref[...]
    for i in range(3):
        piece = rest.astype(BF16)
        rest = rest - piece.astype(F32)
        for tile in range(remote):
            for j in range(sz.slices):
                at = 2 * length + 16 * (i * sz.slices + j)
                part_ref[tile, at : at + 2 * sz.kv_heads, :LANES] = piece[
                    :, j * LANES : (j + 1) * LANES
                ]


def grad_kernel(
    sz, q_ref, own_in_ref, g_ref, far_ref, e_ref, dp_ref, ratio_ref, delta_ref, ds_ref,
    dq_ref, own_ref,
):
    length, remote = sz.length, sz.remote
    sums = {}
    for head in range(sz.kv_heads):
        span, local = sz.span(head), head % 2
        keys = split_halves(own_in_ref[:length, span].astype(F32) * SCALE, local)
        p_near, ds_near, q_rows, g_rows = [], [], [], []

        def far_keys(tile):
            return join(split_halves(far_ref[tile, :length, span].astype(F32) * SCALE, local))

        if remote == 1:
            keys_here = far_keys(0)
            far_keys = lambda tile: keys_here

        for block in range(sz.blocks):
            count = (block + 1) * BLOCK
            at = sz.near_at(block)
            q_rows.append(sz.stack(q_ref, head, block))
            g_rows.append(sz.stack(g_ref, head, block))
            stat = [sz.stat(head, block, half) for half in range(2)]
            ratio = [ratio_ref[r : r + 1] for r in stat]
            delta = [delta_ref[r : r + 1] for r in stat]
            prob = e_ref[head, at] * spread(ratio, count)
            p_near.append(prob.astype(BF16))
            dscore = (prob * (dp_ref[head, at] - spread(delta, count))).astype(BF16)
            ds_near.append(dscore)
            dq = dot(dscore, join([part[:count] for part in keys]), 0, 0)

            def dq_far(tile, carry):
                return carry + dot(ds_ref[head, block, tile], far_keys(tile), 0, 0)

            dq = over_tiles(remote, dq_far, dq)
            for pair in range(sz.pairs):
                dq_ref[sz.rows(block), sz.lanes(head, pair)] = dq[
                    pair * BLOCK : (pair + 1) * BLOCK
                ].astype(BF16)

        for which, parts, right in ((0, ds_near, q_rows), (1, p_near, g_rows)):
            out = [[], []]
            for kb in range(sz.blocks):
                left = []
                for block in range(kb, sz.blocks):
                    left.append(join([half[sz.rows(kb)] for half in halves(parts[block])]))
                for half, total in enumerate(halves(dot(join(left, 1), join(right[kb:]), 1, 0))):
                    out[half].append(total)
            sums[which, local] = [join(o) for o in out]
        if local == 1:
            own_ref[0, :, span] = merge_heads([sums[0, 0], sums[0, 1]]) * SCALE
            own_ref[1, :, span] = merge_heads([sums[1, 0], sums[1, 1]])


def last_kernel(sz, own_ref, back_ref, sinks_ref, dk_ref, dv_ref, out_ref):
    length = sz.length
    totals = [own_ref[0], own_ref[1]]
    sink = sinks_ref[...]
    count = sink.shape[0]
    for tile in range(sz.remote):
        for which in range(2):
            at = slice(which * length, (which + 1) * length)
            totals[which] = totals[which] + back_ref[tile, at].astype(F32)
        rest = jnp.zeros_like(sink)
        for i in range(3):
            pieces = []
            for j in range(sz.slices):
                at = 2 * length + 16 * (i * sz.slices + j)
                pieces.append(back_ref[tile, at : at + count, :LANES].astype(F32))
            rest = rest + join(pieces, 1)
        sink = sink + rest
    dk_ref[...] = totals[0].astype(BF16)
    dv_ref[...] = totals[1].astype(BF16)
    lane = lax.broadcasted_iota(jnp.int32, sink.shape, 1)
    out_lane = lax.broadcasted_iota(jnp.int32, out_ref.shape, 1)
    line = jnp.zeros(out_ref.shape, F32)
    for pair in range(sz.pairs):
        sums = jnp.sum(jnp.where(lane // BLOCK == pair, sink, 0.0), axis=1, keepdims=True)
        for r in range(count):
            at = (r // 2) * 2 * sz.pairs + 2 * pair + r % 2
            line = jnp.where(out_lane == at, sums[r : r + 1], line)
    out_ref[...] = line


def on_device(ctx_size, queries, keys, values, grad_out, segments, sinks):
    sz = Sizes(queries, keys, ctx_size)
    length, width, remote = sz.length, sz.width, sz.remote
    vmem = pl.BlockSpec(memory_space=pltpu.VMEM)
    hbm = pl.BlockSpec(memory_space=pltpu.HBM)
    shape = jax.ShapeDtypeStruct
    seg_line = segments.reshape(1, length)
    small = remote == 1

    def stay(array):
        return pltpu.with_memory_space_constraint(array, pltpu.HBM)

    def params(mib):
        return pltpu.CompilerParams(vmem_limit_bytes=mib << 20)

    def cost(flops):
        return pl.CostEstimate(flops=flops, bytes_accessed=1 << 20, transcendentals=0)

    tile_flops = 4 * queries.shape[0] * queries.shape[1] * length

    packed = pl.pallas_call(
        functools.partial(pack_kernel, sz),
        out_shape=shape((2 * length + 16, sz.cols), BF16),
        in_specs=[hbm, hbm, hbm],
        out_specs=vmem,
        scratch_shapes=[pltpu.VMEM((1, length), jnp.int32)] + [pltpu.SemaphoreType.DMA] * 3,
        compiler_params=params(4),
    )(stay(keys), stay(values), stay(seg_line))

    def turn(array, shift):
        order = [(i, (i + shift) % ctx_size) for i in range(ctx_size)]
        return lax.ppermute(array, "ctx", order)

    far = jnp.stack([turn(packed, s) for s in range(1, ctx_size)])

    q_here, g_here, weights, dprob, tops, mass, feats, sink_in = pl.pallas_call(
        functools.partial(near_kernel, sz),
        out_shape=(
            shape(queries.shape, BF16),
            shape(grad_out.shape, BF16),
            shape((sz.kv_heads, sz.near, width), F32),
            shape((sz.kv_heads, sz.near, width), F32),
            shape((sz.stats, width), F32),
            shape((sz.stats, width), F32),
            shape((length, LANES), BF16),
            shape((2 * sz.kv_heads, width), F32),
        ),
        in_specs=[hbm, hbm, hbm, vmem],
        out_specs=(vmem,) * 8,
        scratch_shapes=[pltpu.SMEM(sinks.shape, F32)] + [pltpu.SemaphoreType.DMA] * 3,
        compiler_params=params(16),
        cost_estimate=cost(2 * tile_flops),
    )(stay(queries), stay(grad_out), stay(sinks), packed)

    part, ds_far, ratio, delta, sink_rows = pl.pallas_call(
        functools.partial(far_kernel, sz, "ctx"),
        out_shape=(
            shape((remote, sz.tall, sz.cols), BF16),
            shape((sz.kv_heads, sz.blocks, remote, 2 * length, width), BF16),
            shape((sz.stats, width), F32),
            shape((sz.stats, width), F32),
            shape((2 * sz.kv_heads, width), F32),
        ),
        in_specs=[vmem] * 9,
        out_specs=(vmem,) * 5,
        scratch_shapes=[
            pltpu.VMEM((1, 8, LANES) if small else (remote, 2 * length, width), F32),
            pltpu.VMEM((1, 8, LANES) if small else (remote, 2 * length, width), F32),
            pltpu.VMEM(
                (sz.blocks, 1, 16, LANES) if small else (sz.blocks, remote, 2 * length, width),
                BF16,
            ),
            pltpu.VMEM((1, 16, LANES) if small else (remote, length, LANES), BF16),
        ],
        compiler_params=params(16 if small else 60),
        cost_estimate=cost(4 * tile_flops),
    )(q_here, g_here, far, sink_in, weights, dprob, tops, mass, feats)

    back = jnp.stack([turn(part[s - 1], -s) for s in range(1, ctx_size)])

    dq, own = pl.pallas_call(
        functools.partial(grad_kernel, sz),
        out_shape=(shape(queries.shape, BF16), shape((2,) + keys.shape, F32)),
        in_specs=[vmem] * 9,
        out_specs=(vmem, vmem),
        compiler_params=params(16 if small else 60),
        cost_estimate=cost(4 * tile_flops),
    )(q_here, packed, g_here, far, weights, dprob, ratio, delta, ds_far)

    heads = sinks.shape[0]
    dk, dv, line = pl.pallas_call(
        functools.partial(last_kernel, sz),
        out_shape=(shape(keys.shape, BF16), shape(values.shape, BF16), shape((1, heads), F32)),
        in_specs=[vmem, vmem, vmem],
        out_specs=(vmem, vmem, vmem),
        compiler_params=params(8),
    )(own, back, sink_rows)
    return dq, dk, dv, line.reshape(heads)


def solution(mesh):
    rows = P(("dp", "ctx"), "tp")
    return jax.shard_map(
        functools.partial(on_device, mesh.shape["ctx"]),
        mesh=mesh,
        in_specs=(rows, rows, rows, rows, P(("dp", "ctx")), P("tp")),
        out_specs=(rows, rows, rows, P(("dp", "tp"))),
        check_vma=False,
    )
```

```python
import functools

import jax
import jax.numpy as jnp
from jax import lax
from jax.experimental import pallas as pl
from jax.experimental.pallas import tpu as pltpu
from jax.sharding import PartitionSpec as P

HEAD_SIZE = 64
LANES = 128
BLOCK = 64
NEG = -1e30
F32 = jnp.float32
BF16 = jnp.bfloat16
SCALE = HEAD_SIZE ** (-0.5)


def dot(left, right, left_dim, right_dim):
    return lax.dot_general(
        left, right, (((left_dim,), (right_dim,)), ((), ())), preferred_element_type=F32
    )


def join(parts, axis=0):
    return parts[0] if len(parts) == 1 else jnp.concatenate(parts, axis=axis)


def over_tiles(count, body, carry):
    if count == 1:
        return body(0, carry)
    return lax.fori_loop(0, count, body, carry)


class Keep:
    def __init__(self, ref, count):
        self.ref, self.inline = ref, count == 1

    def put(self, tile, value):
        if self.inline:
            self.value = value
        else:
            self.ref[tile] = value

    def get(self, tile):
        return self.value if self.inline else self.ref[tile]


class Sizes:
    def __init__(self, queries, keys, ctx_size):
        self.length = queries.shape[0]
        self.kv_heads = keys.shape[1] // HEAD_SIZE
        self.pairs = queries.shape[1] // keys.shape[1] // 2
        self.width = self.pairs * BLOCK
        self.blocks = self.length // BLOCK
        self.remote = ctx_size - 1
        self.cols = keys.shape[1]
        self.near = 2 * BLOCK * self.blocks * (self.blocks + 1) // 2
        self.stats = self.kv_heads * self.blocks * 2
        self.seg_rows = -(-self.length // LANES)
        self.slices = self.width // LANES
        self.extra = 3 * self.slices * 2 * self.kv_heads
        self.tall = 2 * self.length + -(-self.extra // 16) * 16

    def near_at(self, block):
        return slice(BLOCK * block * (block + 1), BLOCK * (block + 1) * (block + 2))

    def stat(self, head, block, half):
        return (head * self.blocks + block) * 2 + half

    def rows(self, block):
        return slice(block * BLOCK, (block + 1) * BLOCK)

    def lanes(self, head, pair):
        at = (head * self.pairs + pair) * LANES
        return slice(at, at + LANES)

    def span(self, head):
        at = head // 2 * LANES
        return slice(at, at + LANES)

    def stack(self, ref, head, block):
        return join([ref[self.rows(block), self.lanes(head, p)] for p in range(self.pairs)])


def columns(row):
    return jnp.broadcast_to(row, (LANES, row.shape[1])).T


def split_halves(block, local):
    lane = lax.broadcasted_iota(jnp.int32, block.shape, 1)
    wide = block.astype(F32)
    turned = pltpu.roll(wide, HEAD_SIZE, 1)
    low = lane < HEAD_SIZE
    zero = jnp.zeros_like(wide)
    if local == 0:
        parts = (jnp.where(low, wide, zero), jnp.where(low, zero, turned))
    else:
        parts = (jnp.where(low, turned, zero), jnp.where(low, zero, wide))
    return [part.astype(BF16) for part in parts]


def seg_features(seg_col, blocked):
    lane = lax.broadcasted_iota(jnp.int32, seg_col.shape, 1)
    other = (lane - BLOCK) != seg_col.astype(jnp.int32)
    if blocked is not None:
        other = other | blocked
    return jnp.where((lane >= BLOCK) & other, NEG, 0.0)


def merge_heads(parts):
    lane = lax.broadcasted_iota(jnp.int32, parts[0][0].shape, 1)
    low = lane < HEAD_SIZE
    (first_low, first_high), (second_low, second_high) = parts
    straight = jnp.where(low, first_low, second_high)
    crossed = jnp.where(low, second_low, first_high)
    return straight + pltpu.roll(crossed, HEAD_SIZE, 1)


def halves(array):
    size = array.shape[0] // 2
    return array[:size], array[size:]


def spread(pair_of_rows, size):
    width = pair_of_rows[0].shape[1]
    return join([jnp.broadcast_to(r, (size, width)) for r in pair_of_rows])


def sink_row(sz, sink_ref, head, half):
    lane = lax.broadcasted_iota(jnp.int32, (1, sz.width), 1)
    line = jnp.zeros((1, sz.width), F32)
    for pair in range(sz.pairs):
        value = sink_ref[head * 2 * sz.pairs + 2 * pair + half]
        line = jnp.where(lane // BLOCK == pair, value, line)
    return line


def pack_kernel(sz, ctx_axis, k_ref, v_ref, seg_ref, out_ref, line_ref, k_sem, v_sem, seg_sem):
    last = lax.axis_index(ctx_axis) == sz.remote

    @pl.when(last)
    def _():
        out_ref[...] = jnp.zeros_like(out_ref)

    @pl.when(jnp.logical_not(last))
    def _():
        seg_copy = pltpu.make_async_copy(seg_ref, line_ref, seg_sem)
        k_copy = pltpu.make_async_copy(k_ref, out_ref.at[pl.ds(0, sz.length)], k_sem)
        v_copy = pltpu.make_async_copy(v_ref, out_ref.at[pl.ds(sz.length, sz.length)], v_sem)
        seg_copy.start()
        k_copy.start()
        v_copy.start()
        seg_copy.wait()
        line = line_ref[...].astype(F32).astype(BF16)
        for i in range(sz.seg_rows):
            count = min(LANES, sz.length - i * LANES)
            at = 2 * sz.length + i
            out_ref[at : at + 1, :count] = line[:, i * LANES : i * LANES + count]
        k_copy.wait()
        v_copy.wait()


def seg_columns(sz, lines):
    lines = lines.astype(F32)
    parts = [columns(lines[i : i + 1, :LANES]) for i in range(sz.seg_rows)]
    return join(parts)[: sz.length]


def near_kernel(
    sz, q_hbm, k_hbm, v_hbm, g_hbm, seg_hbm, sink_hbm, after_ref,
    q_ref, k_ref, g_ref, e_ref, dp_ref, top_ref, mass_ref, feat_ref, sink_rows_ref,
    v_ref, seg_ref, sink_ref, sems,
):
    del after_ref
    pairs_of_refs = (
        (seg_hbm, seg_ref), (sink_hbm, sink_ref), (k_hbm, k_ref),
        (q_hbm, q_ref), (v_hbm, v_ref), (g_hbm, g_ref),
    )
    copies = [
        pltpu.make_async_copy(a, b, sems.at[i]) for i, (a, b) in enumerate(pairs_of_refs)
    ]
    for copy in copies:
        copy.start()
    shape = (sz.length, LANES)
    length = sz.length
    copies[0].wait()
    seg_col = columns(seg_ref[...].astype(F32))
    lane = lax.broadcasted_iota(jnp.int32, shape, 1)
    inner = lax.broadcasted_iota(jnp.int32, shape, 0) % BLOCK
    key_seg = seg_features(seg_col, None)
    key_plain = key_seg.astype(BF16)
    key_diag = jnp.where(lane == inner, 1.0, key_seg).astype(BF16)
    same = (lane - BLOCK) == seg_col.astype(jnp.int32)
    query_feat = jnp.where(
        lane < BLOCK, jnp.where(lane > inner, NEG, 0.0), jnp.where(same, 1.0, 0.0)
    ).astype(BF16)
    feat_ref[...] = query_feat
    for copy in copies[1:]:
        copy.wait()

    for head in range(sz.kv_heads):
        keys = split_halves(k_ref[:, sz.span(head)].astype(F32) * SCALE, head % 2)
        values = split_halves(v_ref[:, sz.span(head)], head % 2)
        sinks = [sink_row(sz, sink_ref, head, half) for half in range(2)]
        for half in range(2):
            sink_rows_ref[2 * head + half : 2 * head + half + 1] = sinks[half]
        for block in range(sz.blocks):
            count = (block + 1) * BLOCK
            rows = sz.rows(block)
            q_wide = join(
                [sz.stack(q_ref, head, block), join([query_feat[rows]] * sz.pairs)], 1
            )
            feats = join(([key_plain[: count - BLOCK]] if block else []) + [key_diag[rows]])
            key_wide = join([join([part[:count] for part in keys]), join([feats, feats])], 1)
            scores = dot(key_wide, q_wide, 1, 1)
            tops = [
                jnp.maximum(jnp.max(part, axis=0, keepdims=True), sinks[half])
                for half, part in enumerate(halves(scores))
            ]
            weight = jnp.exp(scores - spread(tops, count))
            at = sz.near_at(block)
            e_ref[head, at] = weight
            for half, part in enumerate(halves(weight)):
                r = sz.stat(head, block, half)
                top_ref[r : r + 1] = tops[half]
                mass_ref[r : r + 1] = jnp.exp(sinks[half] - tops[half]) + jnp.sum(
                    part, axis=0, keepdims=True
                )
            dp_ref[head, at] = dot(
                join([part[:count] for part in values]), sz.stack(g_ref, head, block), 1, 1
            )


def far_kernel(
    sz, ctx_axis, q_ref, g_ref, far_ref, sink_rows_ref, e_ref, dp_ref, top_ref, mass_ref, feat_ref,
    part_ref, ds_ref, ratio_ref, delta_ref, sinks_out_ref,
    s_keep, dp_keep, p_keep, feat_keep,
):
    length, remote = sz.length, sz.remote
    place = lax.axis_index(ctx_axis)
    query_feat = feat_ref[...]
    far_feat = Keep(feat_keep, remote)

    def make_feat(tile, carry):
        far_col = seg_columns(sz, far_ref[tile][2 * length :])
        gone = jnp.full((length, LANES), place - 1 - tile) < 0
        far_feat.put(tile, seg_features(far_col, gone).astype(BF16))
        return carry

    over_tiles(remote, make_feat, 0)
    sums = {}

    for head in range(sz.kv_heads):
        span, local = sz.span(head), head % 2
        q_rows = [sz.stack(q_ref, head, block) for block in range(sz.blocks)]
        g_rows = [sz.stack(g_ref, head, block) for block in range(sz.blocks)]
        sinks = [sink_rows_ref[2 * head + half : 2 * head + half + 1] for half in range(2)]
        sink_sums = [0.0, 0.0]
        far_p = [Keep(p_keep.at[block], remote) for block in range(sz.blocks)]
        far_ds = [Keep(ds_ref.at[head, block], remote) for block in range(sz.blocks)]

        def far_keys(tile):
            return join(split_halves(far_ref[tile, :length, span].astype(F32) * SCALE, local))

        def far_values(tile):
            return join(split_halves(far_ref[tile, length : 2 * length, span], local))

        if remote == 1:
            keys_here, values_here = far_keys(0), far_values(0)
            far_keys, far_values = (lambda tile: keys_here), (lambda tile: values_here)

        for block in range(sz.blocks):
            count = (block + 1) * BLOCK
            q_wide = join([q_rows[block], join([query_feat[sz.rows(block)]] * sz.pairs)], 1)
            g_stack = g_rows[block]
            far_s, far_dp = Keep(s_keep, remote), Keep(dp_keep, remote)
            stat = [sz.stat(head, block, half) for half in range(2)]
            near_tops = [top_ref[r : r + 1] for r in stat]

            def score_far(tile, carry):
                feats = far_feat.get(tile)
                wide = join([far_keys(tile), join([feats, feats])], 1)
                scores = dot(wide, q_wide, 1, 1)
                far_s.put(tile, scores)
                return tuple(
                    jnp.maximum(c, jnp.max(part, axis=0, keepdims=True))
                    for c, part in zip(carry, halves(scores))
                )

            tops = over_tiles(remote, score_far, tuple(near_tops))
            shrink = [jnp.exp(near_tops[half] - tops[half]) for half in range(2)]
            mass = tuple(mass_ref[r : r + 1] * s for r, s in zip(stat, shrink))

            def mass_far(tile, carry):
                weight = jnp.exp(far_s.get(tile) - spread(tops, length))
                far_s.put(tile, weight)
                return tuple(
                    c + jnp.sum(part, axis=0, keepdims=True)
                    for c, part in zip(carry, halves(weight))
                )

            mass = over_tiles(remote, mass_far, mass)
            inverse = [1.0 / m for m in mass]
            ratio = [s * i for s, i in zip(shrink, inverse)]
            at = sz.near_at(block)
            near_half = (e_ref[head, at] * spread(ratio, count)).astype(BF16)
            prod = near_half.astype(F32) * dp_ref[head, at]
            delta = tuple(jnp.sum(part, axis=0, keepdims=True) for part in halves(prod))

            def delta_far(tile, carry):
                prob = far_s.get(tile) * spread(inverse, length)
                far_s.put(tile, prob)
                rounded = prob.astype(BF16)
                far_p[block].put(tile, rounded)
                dprob = dot(far_values(tile), g_stack, 1, 1)
                far_dp.put(tile, dprob)
                return tuple(
                    c + jnp.sum(part, axis=0, keepdims=True)
                    for c, part in zip(carry, halves(rounded.astype(F32) * dprob))
                )

            delta = over_tiles(remote, delta_far, delta)
            for half in range(2):
                sink_prob = jnp.exp(sinks[half] - tops[half]) * inverse[half]
                sink_sums[half] = sink_sums[half] - sink_prob * delta[half]
                ratio_ref[stat[half] : stat[half] + 1] = ratio[half]
                delta_ref[stat[half] : stat[half] + 1] = delta[half]

            def dscore_far(tile, carry):
                dscore = far_s.get(tile) * (far_dp.get(tile) - spread(delta, length))
                dscore = dscore.astype(BF16)
                far_ds[block].put(tile, dscore)
                if remote == 1:
                    ds_ref[head, block, tile] = dscore
                return carry

            over_tiles(remote, dscore_far, 0)

        for half in range(2):
            sinks_out_ref[2 * head + half : 2 * head + half + 1, :] = sink_sums[half]
        q_all, g_all = join(q_rows), join(g_rows)

        def far_sum(tile, carry):
            for which, parts, right in ((0, far_ds, q_all), (1, far_p, g_all)):
                total = dot(join([part.get(tile) for part in parts], 1), right, 1, 0)
                if remote == 1:
                    sums[which, local] = halves(total)
                else:
                    at = slice(which * length, (which + 1) * length)
                    lane = lax.broadcasted_iota(jnp.int32, (length, LANES), 1)
                    low = lane < HEAD_SIZE
                    a, b = halves(total)
                    turned = pltpu.roll(jnp.where(low, a, b), HEAD_SIZE, 1)
                    both = ((a if local == 0 else b) + turned) * (SCALE if which == 0 else 1.0)
                    keep = low if local == 0 else ~low
                    part_ref[tile, at, span] = jnp.where(
                        keep, both.astype(BF16), part_ref[tile, at, span]
                    )
            return carry

        over_tiles(remote, far_sum, 0)
        if remote == 1 and local == 1:
            for which, factor in ((0, SCALE), (1, 1.0)):
                merged = merge_heads([sums[which, 0], sums[which, 1]]) * factor
                part_ref[0, which * length : (which + 1) * length, span] = merged.astype(BF16)

    rest = sinks_out_ref[...]
    for i in range(3):
        piece = rest.astype(BF16)
        rest = rest - piece.astype(F32)
        for tile in range(remote):
            for j in range(sz.slices):
                at = 2 * length + 2 * sz.kv_heads * (i * sz.slices + j)
                part_ref[tile, at : at + 2 * sz.kv_heads, :LANES] = piece[
                    :, j * LANES : (j + 1) * LANES
                ]


def grad_kernel(
    sz, q_ref, k_ref, g_ref, far_ref, e_ref, dp_ref, ratio_ref, delta_ref, ds_ref,
    dq_ref, own_ref,
):
    length, remote = sz.length, sz.remote
    sums = {}
    for head in range(sz.kv_heads):
        span, local = sz.span(head), head % 2
        keys = split_halves(k_ref[:, span].astype(F32) * SCALE, local)
        p_near, ds_near, q_rows, g_rows = [], [], [], []

        def far_keys(tile):
            return join(split_halves(far_ref[tile, :length, span].astype(F32) * SCALE, local))

        if remote == 1:
            keys_here = far_keys(0)
            far_keys = lambda tile: keys_here

        for block in range(sz.blocks):
            count = (block + 1) * BLOCK
            at = sz.near_at(block)
            q_rows.append(sz.stack(q_ref, head, block))
            g_rows.append(sz.stack(g_ref, head, block))
            stat = [sz.stat(head, block, half) for half in range(2)]
            ratio = [ratio_ref[r : r + 1] for r in stat]
            delta = [delta_ref[r : r + 1] for r in stat]
            prob = e_ref[head, at] * spread(ratio, count)
            p_near.append(prob.astype(BF16))
            dscore = (prob * (dp_ref[head, at] - spread(delta, count))).astype(BF16)
            ds_near.append(dscore)
            dq = dot(dscore, join([part[:count] for part in keys]), 0, 0)

            def dq_far(tile, carry):
                return carry + dot(ds_ref[head, block, tile], far_keys(tile), 0, 0)

            dq = over_tiles(remote, dq_far, dq)
            for pair in range(sz.pairs):
                dq_ref[sz.rows(block), sz.lanes(head, pair)] = dq[
                    pair * BLOCK : (pair + 1) * BLOCK
                ].astype(BF16)

        for which, parts, right in ((0, ds_near, q_rows), (1, p_near, g_rows)):
            out = [[], []]
            for kb in range(sz.blocks):
                left = []
                for block in range(kb, sz.blocks):
                    left.append(join([half[sz.rows(kb)] for half in halves(parts[block])]))
                for half, total in enumerate(halves(dot(join(left, 1), join(right[kb:]), 1, 0))):
                    out[half].append(total)
            sums[which, local] = [join(o) for o in out]
        if local == 1:
            own_ref[0, :, span] = merge_heads([sums[0, 0], sums[0, 1]]) * SCALE
            own_ref[1, :, span] = merge_heads([sums[1, 0], sums[1, 1]])


def last_kernel(sz, own_ref, back_ref, sinks_ref, dk_ref, dv_ref, out_ref):
    length = sz.length
    totals = [own_ref[0], own_ref[1]]
    sink = sinks_ref[...]
    count = sink.shape[0]
    for tile in range(sz.remote):
        for which in range(2):
            at = slice(which * length, (which + 1) * length)
            totals[which] = totals[which] + back_ref[tile, at].astype(F32)
        rest = jnp.zeros_like(sink)
        for i in range(3):
            pieces = []
            for j in range(sz.slices):
                at = 2 * length + count * (i * sz.slices + j)
                pieces.append(back_ref[tile, at : at + count, :LANES].astype(F32))
            rest = rest + join(pieces, 1)
        sink = sink + rest
    dk_ref[...] = totals[0].astype(BF16)
    dv_ref[...] = totals[1].astype(BF16)
    lane = lax.broadcasted_iota(jnp.int32, sink.shape, 1)
    out_lane = lax.broadcasted_iota(jnp.int32, out_ref.shape, 1)
    line = jnp.zeros(out_ref.shape, F32)
    for pair in range(sz.pairs):
        sums = jnp.sum(jnp.where(lane // BLOCK == pair, sink, 0.0), axis=1, keepdims=True)
        for r in range(count):
            at = (r // 2) * 2 * sz.pairs + 2 * pair + r % 2
            line = jnp.where(out_lane == at, sums[r : r + 1], line)
    out_ref[...] = line


def on_device(ctx_size, queries, keys, values, grad_out, segments, sinks):
    sz = Sizes(queries, keys, ctx_size)
    length, width, remote = sz.length, sz.width, sz.remote
    vmem = pl.BlockSpec(memory_space=pltpu.VMEM)
    hbm = pl.BlockSpec(memory_space=pltpu.HBM)
    shape = jax.ShapeDtypeStruct
    seg_line = segments.reshape(1, length)
    small = remote == 1

    def stay(array):
        return pltpu.with_memory_space_constraint(array, pltpu.HBM)

    def params(mib):
        return pltpu.CompilerParams(vmem_limit_bytes=mib << 20)

    def cost(flops):
        return pl.CostEstimate(flops=flops, bytes_accessed=1 << 20, transcendentals=0)

    tile_flops = 4 * queries.shape[0] * queries.shape[1] * length

    packed = pl.pallas_call(
        functools.partial(pack_kernel, sz, "ctx"),
        name="pack",
        out_shape=shape((2 * length + 16, sz.cols), BF16),
        in_specs=[hbm, hbm, hbm],
        out_specs=vmem,
        scratch_shapes=[pltpu.VMEM((1, length), jnp.int32)] + [pltpu.SemaphoreType.DMA] * 3,
        compiler_params=params(4),
    )(stay(keys), stay(values), stay(seg_line))

    def turn(array, shift):
        order = [(i, (i + shift) % ctx_size) for i in range(ctx_size)]
        return lax.ppermute(array, "ctx", order)

    far = jnp.stack([turn(packed, s) for s in range(1, ctx_size)])

    q_here, k_here, g_here, weights, dprob, tops, mass, feats, sink_in = pl.pallas_call(
        functools.partial(near_kernel, sz),
        name="near",
        out_shape=(
            shape(queries.shape, BF16),
            shape(keys.shape, BF16),
            shape(grad_out.shape, BF16),
            shape((sz.kv_heads, sz.near, width), F32),
            shape((sz.kv_heads, sz.near, width), F32),
            shape((sz.stats, width), F32),
            shape((sz.stats, width), F32),
            shape((length, LANES), BF16),
            shape((2 * sz.kv_heads, width), F32),
        ),
        in_specs=[hbm] * 6 + [vmem],
        out_specs=(vmem,) * 9,
        scratch_shapes=[
            pltpu.VMEM(values.shape, BF16),
            pltpu.VMEM((1, length), jnp.int32),
            pltpu.SMEM(sinks.shape, F32),
            pltpu.SemaphoreType.DMA((6,)),
        ],
        compiler_params=params(16),
        cost_estimate=cost(2 * tile_flops),
    )(*[stay(a) for a in (queries, keys, values, grad_out, seg_line, sinks)], packed)

    part, ds_far, ratio, delta, sink_rows = pl.pallas_call(
        functools.partial(far_kernel, sz, "ctx"),
        name="far",
        out_shape=(
            shape((remote, sz.tall, sz.cols), BF16),
            shape((sz.kv_heads, sz.blocks, remote, 2 * length, width), BF16),
            shape((sz.stats, width), F32),
            shape((sz.stats, width), F32),
            shape((2 * sz.kv_heads, width), F32),
        ),
        in_specs=[vmem] * 9,
        out_specs=(vmem,) * 5,
        scratch_shapes=[
            pltpu.VMEM((1, 8, LANES) if small else (remote, 2 * length, width), F32),
            pltpu.VMEM((1, 8, LANES) if small else (remote, 2 * length, width), F32),
            pltpu.VMEM(
                (sz.blocks, 1, 16, LANES) if small else (sz.blocks, remote, 2 * length, width),
                BF16,
            ),
            pltpu.VMEM((1, 16, LANES) if small else (remote, length, LANES), BF16),
        ],
        compiler_params=params(16 if small else 60),
        cost_estimate=cost(4 * tile_flops),
    )(q_here, g_here, far, sink_in, weights, dprob, tops, mass, feats)

    back = jnp.stack([turn(part[s - 1], -s) for s in range(1, ctx_size)])

    dq, own = pl.pallas_call(
        functools.partial(grad_kernel, sz),
        name="grad",
        out_shape=(shape(queries.shape, BF16), shape((2,) + keys.shape, F32)),
        in_specs=[vmem] * 9,
        out_specs=(vmem, vmem),
        compiler_params=params(16 if small else 60),
        cost_estimate=cost(4 * tile_flops),
    )(q_here, k_here, g_here, far, weights, dprob, ratio, delta, ds_far)

    heads = sinks.shape[0]
    dk, dv, line = pl.pallas_call(
        functools.partial(last_kernel, sz),
        name="last",
        out_shape=(shape(keys.shape, BF16), shape(values.shape, BF16), shape((1, heads), F32)),
        in_specs=[vmem, vmem, vmem],
        out_specs=(vmem, vmem, vmem),
        compiler_params=params(8),
    )(own, back, sink_rows)
    return dq, dk, dv, line.reshape(heads)


def solution(mesh):
    rows = P(("dp", "ctx"), "tp")
    return jax.shard_map(
        functools.partial(on_device, mesh.shape["ctx"]),
        mesh=mesh,
        in_specs=(rows, rows, rows, rows, P(("dp", "ctx")), P("tp")),
        out_specs=(rows, rows, rows, P(("dp", "tp"))),
        check_vma=False,
    )
```

```python
import functools

import jax
import jax.numpy as jnp
from jax import lax
from jax.experimental import pallas as pl
from jax.experimental.pallas import tpu as pltpu
from jax.sharding import PartitionSpec as P

HEAD_SIZE = 64
LANES = 128
BLOCK = 64
NEG = -1e30
F32 = jnp.float32
BF16 = jnp.bfloat16
SCALE = HEAD_SIZE ** (-0.5)


def dot(left, right, left_dim, right_dim):
    return lax.dot_general(
        left, right, (((left_dim,), (right_dim,)), ((), ())), preferred_element_type=F32
    )


def join(parts, axis=0):
    return parts[0] if len(parts) == 1 else jnp.concatenate(parts, axis=axis)


class Sizes:
    def __init__(self, queries, keys, ctx_size):
        self.length = queries.shape[0]
        self.kv_heads = keys.shape[1] // HEAD_SIZE
        self.pairs = queries.shape[1] // keys.shape[1] // 2
        self.width = self.pairs * BLOCK
        self.blocks = self.length // BLOCK
        self.remote = ctx_size - 1
        self.cols = keys.shape[1]
        self.near = 2 * BLOCK * self.blocks * (self.blocks + 1) // 2
        self.stats = self.kv_heads * self.blocks * 2
        self.seg_rows = -(-self.length // LANES)
        self.slices = self.width // LANES
        self.extra = 3 * self.slices * 2 * self.kv_heads
        self.tall = 2 * self.length + -(-self.extra // 16) * 16

    def near_at(self, block):
        return slice(BLOCK * block * (block + 1), BLOCK * (block + 1) * (block + 2))

    def stat(self, head, block, half):
        return (head * self.blocks + block) * 2 + half

    def rows(self, block):
        return slice(block * BLOCK, (block + 1) * BLOCK)

    def lanes(self, head, pair):
        at = (head * self.pairs + pair) * LANES
        return slice(at, at + LANES)

    def span(self, head):
        at = head // 2 * LANES
        return slice(at, at + LANES)


def columns(row):
    return jnp.broadcast_to(row, (LANES, row.shape[1])).T


def split_halves(block, local):
    lane = lax.broadcasted_iota(jnp.int32, block.shape, 1)
    wide = block.astype(F32)
    turned = pltpu.roll(wide, HEAD_SIZE, 1)
    low = lane < HEAD_SIZE
    zero = jnp.zeros_like(wide)
    if local == 0:
        parts = (jnp.where(low, wide, zero), jnp.where(low, zero, turned))
    else:
        parts = (jnp.where(low, turned, zero), jnp.where(low, zero, wide))
    return [part.astype(BF16) for part in parts]


def seg_features(seg_col, blocked):
    lane = lax.broadcasted_iota(jnp.int32, seg_col.shape, 1)
    other = (lane - BLOCK) != seg_col.astype(jnp.int32)
    if blocked is not None:
        other = other | blocked
    return jnp.where((lane >= BLOCK) & other, NEG, 0.0)


def merge_heads(parts):
    lane = lax.broadcasted_iota(jnp.int32, parts[0][0].shape, 1)
    low = lane < HEAD_SIZE
    (first_low, first_high), (second_low, second_high) = parts
    straight = jnp.where(low, first_low, second_high)
    crossed = jnp.where(low, second_low, first_high)
    return straight + pltpu.roll(crossed, HEAD_SIZE, 1)


def halves(array):
    size = array.shape[0] // 2
    return array[:size], array[size:]


def fold(array, reduce):
    return reduce(array.reshape(array.shape[0] // 8, 8, array.shape[1]), axis=0)


def row_sum(tile):
    return jnp.sum(tile, axis=0, keepdims=True)


def row_max(tile):
    return jnp.max(tile, axis=0, keepdims=True)


def spread(pair_of_rows, size):
    width = pair_of_rows[0].shape[1]
    return join([jnp.broadcast_to(r, (size, width)) for r in pair_of_rows])


def sink_row(sz, sink_ref, head, half):
    lane = lax.broadcasted_iota(jnp.int32, (1, sz.width), 1)
    line = jnp.zeros((1, sz.width), F32)
    for pair in range(sz.pairs):
        value = sink_ref[head * 2 * sz.pairs + 2 * pair + half]
        line = jnp.where(lane // BLOCK == pair, value, line)
    return line


def pack_kernel(
    sz, ctx_axis, k_ref, v_ref, seg_ref, out_k_ref, out_v_ref, line_ref, k_sem, v_sem, seg_sem
):
    last = lax.axis_index(ctx_axis) == sz.remote

    @pl.when(last)
    def _():
        out_k_ref[...] = jnp.zeros_like(out_k_ref)
        out_v_ref[...] = jnp.zeros_like(out_v_ref)

    @pl.when(jnp.logical_not(last))
    def _():
        seg_copy = pltpu.make_async_copy(seg_ref, line_ref, seg_sem)
        k_copy = pltpu.make_async_copy(k_ref, out_k_ref.at[pl.ds(0, sz.length)], k_sem)
        v_copy = pltpu.make_async_copy(v_ref, out_v_ref, v_sem)
        seg_copy.start()
        k_copy.start()
        v_copy.start()
        seg_copy.wait()
        line = line_ref[...].astype(F32).astype(BF16)
        for i in range(sz.seg_rows):
            count = min(LANES, sz.length - i * LANES)
            at = sz.length + i
            out_k_ref[at : at + 1, :count] = line[:, i * LANES : i * LANES + count]
        k_copy.wait()
        v_copy.wait()


def seg_columns(sz, lines):
    lines = lines.astype(F32)
    parts = [columns(lines[i : i + 1, :LANES]) for i in range(sz.seg_rows)]
    return join(parts)[: sz.length]


def near_kernel(
    sz, q_hbm, k_hbm, v_hbm, g_hbm, seg_hbm, sink_hbm, after_k_ref, after_v_ref,
    q_ref, k_ref, g_ref, e_ref, dp_ref, top_ref, mass_ref, feat_ref, sink_rows_ref,
    q_flat, g_flat, v_ref, seg_ref, sink_ref, sems,
):
    del after_k_ref, after_v_ref
    pairs_of_refs = (
        (seg_hbm, seg_ref), (sink_hbm, sink_ref), (k_hbm, k_ref),
        (q_hbm, q_flat), (v_hbm, v_ref), (g_hbm, g_flat),
    )
    copies = [
        pltpu.make_async_copy(a, b, sems.at[i]) for i, (a, b) in enumerate(pairs_of_refs)
    ]
    for copy in copies:
        copy.start()

    def stack(ref, head, block):
        return join([ref[sz.rows(block), sz.lanes(head, pair)] for pair in range(sz.pairs)])

    shape = (sz.length, LANES)
    copies[0].wait()
    seg_col = columns(seg_ref[...].astype(F32))
    lane = lax.broadcasted_iota(jnp.int32, shape, 1)
    inner = lax.broadcasted_iota(jnp.int32, shape, 0) % BLOCK
    key_seg = seg_features(seg_col, None)
    key_plain = key_seg.astype(BF16)
    key_diag = jnp.where(lane == inner, 1.0, key_seg).astype(BF16)
    same = (lane - BLOCK) == seg_col.astype(jnp.int32)
    query_feat = jnp.where(
        lane < BLOCK, jnp.where(lane > inner, NEG, 0.0), jnp.where(same, 1.0, 0.0)
    ).astype(BF16)
    feat_ref[...] = query_feat
    for copy in copies[1:]:
        copy.wait()

    for head in range(sz.kv_heads):
        keys = split_halves(k_ref[:, sz.span(head)].astype(F32) * SCALE, head % 2)
        values = split_halves(v_ref[:, sz.span(head)], head % 2)
        sinks = [sink_row(sz, sink_ref, head, half) for half in range(2)]
        for half in range(2):
            sink_rows_ref[2 * head + half : 2 * head + half + 1] = sinks[half]
        for block in range(sz.blocks):
            count = (block + 1) * BLOCK
            rows = sz.rows(block)
            q_stack = stack(q_flat, head, block)
            q_ref[head, block] = q_stack
            q_wide = join([q_stack, join([query_feat[rows]] * sz.pairs)], 1)
            feats = join(([key_plain[: count - BLOCK]] if block else []) + [key_diag[rows]])
            key_wide = join([join([part[:count] for part in keys]), join([feats, feats])], 1)
            scores = dot(key_wide, q_wide, 1, 1)
            tops = [
                jnp.maximum(row_max(fold(part, jnp.max)), sinks[half])
                for half, part in enumerate(halves(scores))
            ]
            weight = jnp.exp(scores - spread(tops, count))
            at = sz.near_at(block)
            e_ref[head, at] = weight
            for half, part in enumerate(halves(weight)):
                r = sz.stat(head, block, half)
                top_ref[r : r + 1] = tops[half]
                mass_ref[r : r + 1] = jnp.exp(sinks[half] - tops[half]) + row_sum(
                    fold(part, jnp.sum)
                )
            g_stack = stack(g_flat, head, block)
            g_ref[head, block] = g_stack
            dp_ref[head, at] = dot(join([part[:count] for part in values]), g_stack, 1, 1)


def far_features(sz, far_k_ref, tile):
    seg_col = seg_columns(sz, far_k_ref[tile, sz.length :])
    feats = seg_features(seg_col, None).astype(BF16)
    return join([feats, feats])


def far_scores(sz, far_k_ref, q_ref, query_feat, head, block, tile, feats):
    keys = split_halves(far_k_ref[tile, : sz.length, sz.span(head)].astype(F32) * SCALE, head % 2)
    q_wide = join([q_ref[head, block], join([query_feat[sz.rows(block)]] * sz.pairs)], 1)
    return dot(join([join(keys), feats], 1), q_wide, 1, 1)


def stat_kernel(
    sz, ctx_axis, q_ref, far_k_ref, sink_rows_ref, top_ref, mass_ref, feat_ref,
    e_far_ref, top_out_ref, ratio_ref, inverse_ref, sink_prob_ref,
):
    place = lax.axis_index(ctx_axis)
    query_feat = feat_ref[...]

    def finish(head, block, half, top, mass):
        r = sz.stat(head, block, half)
        inverse = 1.0 / mass
        top_out_ref[r : r + 1] = top
        inverse_ref[r : r + 1] = inverse
        ratio_ref[r : r + 1] = jnp.exp(top_ref[r : r + 1] - top) * inverse
        sink = sink_rows_ref[2 * head + half : 2 * head + half + 1]
        sink_prob_ref[r : r + 1] = jnp.exp(sink - top) * inverse

    def each(body):
        for head in range(sz.kv_heads):
            for block in range(sz.blocks):
                body(head, block, [sz.stat(head, block, half) for half in range(2)])

    def inline():
        feats = far_features(sz, far_k_ref, 0)

        def body(head, block, stat):
            scores = far_scores(sz, far_k_ref, q_ref, query_feat, head, block, 0, feats)
            near_tops = [top_ref[r : r + 1] for r in stat]
            tops = [
                jnp.maximum(near, row_max(fold(part, jnp.max)))
                for near, part in zip(near_tops, halves(scores))
            ]
            weight = jnp.exp(scores - spread(tops, sz.length))
            e_far_ref[head, block] = weight
            for half, part in enumerate(halves(weight)):
                shrunk = mass_ref[stat[half] : stat[half] + 1] * jnp.exp(
                    near_tops[half] - tops[half]
                )
                finish(head, block, half, tops[half], shrunk + row_sum(fold(part, jnp.sum)))

        each(body)

    def looped(count):
        def body(head, block, stat):
            def step(tile, carry):
                feats = far_features(sz, far_k_ref, tile)
                scores = far_scores(sz, far_k_ref, q_ref, query_feat, head, block, tile, feats)
                tops, masses = carry
                new = tuple(
                    jnp.maximum(old, row_max(part)) for old, part in zip(tops, halves(scores))
                )
                weight = jnp.exp(scores - spread(new, sz.length))
                return new, tuple(
                    mass * jnp.exp(old - top) + row_sum(part)
                    for mass, old, top, part in zip(masses, tops, new, halves(weight))
                )

            start = (
                tuple(top_ref[r : r + 1] for r in stat),
                tuple(mass_ref[r : r + 1] for r in stat),
            )
            tops, masses = lax.fori_loop(0, count, step, start)
            for half in range(2):
                finish(head, block, half, tops[half], masses[half])

        each(body)

    if sz.remote == 1:

        @pl.when(place > 0)
        def _():
            inline()

        @pl.when(place == 0)
        def _():
            looped(0)

    else:
        looped(place)


def far_kernel(
    sz, ctx_axis, q_ref, g_ref, far_k_ref, far_v_ref, e_ref, dp_ref, feat_ref,
    e_far_ref, top_ref, ratio_ref, inverse_ref, sink_prob_ref,
    part_ref, ds_ref, delta_ref, sinks_out_ref,
    s_keep, dp_keep, p_keep,
):
    length, remote = sz.length, sz.remote
    place = lax.axis_index(ctx_axis)
    query_feat = feat_ref[...]

    def near_delta(head, block, ratio):
        at = sz.near_at(block)
        rounded = (e_ref[head, at] * spread(ratio, (block + 1) * BLOCK)).astype(BF16)
        prod = rounded.astype(F32) * dp_ref[head, at]
        return tuple(fold(part, jnp.sum) for part in halves(prod))

    def rows_of(ref, head, block):
        return [ref[r : r + 1] for r in (sz.stat(head, block, half) for half in range(2))]

    def finish(head, block, delta, sink_sums):
        for half, sink_prob in enumerate(rows_of(sink_prob_ref, head, block)):
            r = sz.stat(head, block, half)
            delta_ref[r : r + 1] = delta[half]
            sink_sums[half] = sink_sums[half] - sink_prob * delta[half]

    def put_sinks(head, sink_sums):
        for half in range(2):
            sinks_out_ref[2 * head + half : 2 * head + half + 1, :] = sink_sums[half]

    def values_of(head, tile):
        return join(split_halves(far_v_ref[tile, :, sz.span(head)], head % 2))

    def inline():
        sums = {}
        for head in range(sz.kv_heads):
            values = values_of(head, 0)
            sink_sums = [0.0, 0.0]
            p_far, ds_far = [], []
            for block in range(sz.blocks):
                delta = near_delta(head, block, rows_of(ratio_ref, head, block))
                dprob = dot(values, g_ref[head, block], 1, 1)
                prob = e_far_ref[head, block] * spread(rows_of(inverse_ref, head, block), length)
                rounded = prob.astype(BF16)
                p_far.append(rounded)
                delta = [
                    row_sum(near + fold(part, jnp.sum))
                    for near, part in zip(delta, halves(rounded.astype(F32) * dprob))
                ]
                finish(head, block, delta, sink_sums)
                dscore = (prob * (dprob - spread(delta, length))).astype(BF16)
                ds_far.append(dscore)
                for j in range(sz.slices):
                    ds_ref[head, block, 0, j] = dscore[:, j * LANES : (j + 1) * LANES]
            put_sinks(head, sink_sums)
            for which, parts, ref in ((0, ds_far, q_ref), (1, p_far, g_ref)):
                right = join([ref[head, block] for block in range(sz.blocks)])
                sums[which, head % 2] = halves(dot(join(parts, 1), right, 1, 0))
            if head % 2 == 1:
                for which, factor in ((0, SCALE), (1, 1.0)):
                    merged = merge_heads([sums[which, 0], sums[which, 1]]) * factor
                    rows = slice(which * length, (which + 1) * length)
                    part_ref[0, rows, sz.span(head)] = merged.astype(BF16)

    def looped(count):
        part_ref[:, : 2 * length] = jnp.zeros_like(part_ref[:, : 2 * length])
        for head in range(sz.kv_heads):
            span, local = sz.span(head), head % 2
            sink_sums = [0.0, 0.0]
            for block in range(sz.blocks):
                delta = near_delta(head, block, rows_of(ratio_ref, head, block))
                delta = tuple(row_sum(part) for part in delta)
                tops = rows_of(top_ref, head, block)
                inverse = rows_of(inverse_ref, head, block)

                def prob_far(tile, carry):
                    feats = far_features(sz, far_k_ref, tile)
                    scores = far_scores(
                        sz, far_k_ref, q_ref, query_feat, head, block, tile, feats
                    )
                    prob = jnp.exp(scores - spread(tops, length)) * spread(inverse, length)
                    rounded = prob.astype(BF16)
                    dprob = dot(values_of(head, tile), g_ref[head, block], 1, 1)
                    s_keep[tile] = prob
                    dp_keep[tile] = dprob
                    p_keep[block, tile] = rounded
                    return tuple(
                        c + row_sum(part)
                        for c, part in zip(carry, halves(rounded.astype(F32) * dprob))
                    )

                if remote > 1:
                    delta = lax.fori_loop(0, count, prob_far, delta)
                finish(head, block, delta, sink_sums)

                def dscore_far(tile, carry):
                    dscore = (s_keep[tile] * (dp_keep[tile] - spread(delta, length))).astype(BF16)
                    for j in range(sz.slices):
                        ds_ref[head, block, tile, j] = dscore[:, j * LANES : (j + 1) * LANES]
                    return carry

                if remote > 1:
                    lax.fori_loop(0, count, dscore_far, 0)
            put_sinks(head, sink_sums)

            def far_sum(tile, carry):
                for which, ref in ((0, q_ref), (1, g_ref)):
                    total = jnp.zeros((2 * length, LANES), F32)
                    for block in range(sz.blocks):
                        left = p_keep[block, tile]
                        if which == 0:
                            left = join([ds_ref[head, block, tile, j] for j in range(sz.slices)], 1)
                        total = total + dot(left, ref[head, block], 1, 0)
                    at = slice(which * length, (which + 1) * length)
                    lane = lax.broadcasted_iota(jnp.int32, (length, LANES), 1)
                    low = lane < HEAD_SIZE
                    a, b = halves(total)
                    turned = pltpu.roll(jnp.where(low, a, b), HEAD_SIZE, 1)
                    both = ((a if local == 0 else b) + turned) * (SCALE if which == 0 else 1.0)
                    keep = low if local == 0 else ~low
                    part_ref[tile, at, span] = jnp.where(
                        keep, both.astype(BF16), part_ref[tile, at, span]
                    )
                return carry

            if remote > 1:
                lax.fori_loop(0, count, far_sum, 0)

    if remote == 1:

        @pl.when(place > 0)
        def _():
            inline()

        @pl.when(place == 0)
        def _():
            looped(0)
            ds_ref[...] = jnp.zeros_like(ds_ref)

    else:
        looped(place)

    rest = sinks_out_ref[...]
    for i in range(3):
        piece = rest.astype(BF16)
        rest = rest - piece.astype(F32)
        for tile in range(remote):
            for j in range(sz.slices):
                at = 2 * length + 2 * sz.kv_heads * (i * sz.slices + j)
                part_ref[tile, at : at + 2 * sz.kv_heads, :LANES] = piece[
                    :, j * LANES : (j + 1) * LANES
                ]


def grad_kernel(
    sz, ctx_axis, q_ref, k_ref, g_ref, far_k_ref, e_ref, dp_ref, ratio_ref, delta_ref, ds_ref,
    dq_ref, own_ref,
):
    length, remote = sz.length, sz.remote
    place = lax.axis_index(ctx_axis)
    sums = {}
    for head in range(sz.kv_heads):
        span, local = sz.span(head), head % 2
        keys = split_halves(k_ref[:, span].astype(F32) * SCALE, local)
        p_near, ds_near, q_rows, g_rows = [], [], [], []

        def far_keys(tile):
            return join(split_halves(far_k_ref[tile, :length, span].astype(F32) * SCALE, local))

        if remote == 1:
            keys_here = far_keys(0)

        for block in range(sz.blocks):
            count = (block + 1) * BLOCK
            at = sz.near_at(block)
            q_rows.append(q_ref[head, block])
            g_rows.append(g_ref[head, block])
            stat = [sz.stat(head, block, half) for half in range(2)]
            ratio = [ratio_ref[r : r + 1] for r in stat]
            delta = [delta_ref[r : r + 1] for r in stat]
            prob = e_ref[head, at] * spread(ratio, count)
            p_near.append(prob.astype(BF16))
            dscore = (prob * (dp_ref[head, at] - spread(delta, count))).astype(BF16)
            ds_near.append(dscore)
            dq = dot(dscore, join([part[:count] for part in keys]), 0, 0)

            def ds_far(tile):
                return join([ds_ref[head, block, tile, j] for j in range(sz.slices)], 1)

            if remote == 1:
                dq = dq + dot(ds_far(0), keys_here, 0, 0)
            else:
                dq = lax.fori_loop(
                    0, place, lambda tile, c: c + dot(ds_far(tile), far_keys(tile), 0, 0), dq
                )
            for pair in range(sz.pairs):
                dq_ref[sz.rows(block), sz.lanes(head, pair)] = dq[
                    pair * BLOCK : (pair + 1) * BLOCK
                ].astype(BF16)

        for which, parts, right in ((0, ds_near, q_rows), (1, p_near, g_rows)):
            out = [[], []]
            for kb in range(sz.blocks):
                left = []
                for block in range(kb, sz.blocks):
                    left.append(join([half[sz.rows(kb)] for half in halves(parts[block])]))
                for half, total in enumerate(halves(dot(join(left, 1), join(right[kb:]), 1, 0))):
                    out[half].append(total)
            sums[which, local] = [join(o) for o in out]
        if local == 1:
            own_ref[0, :, span] = merge_heads([sums[0, 0], sums[0, 1]]) * SCALE
            own_ref[1, :, span] = merge_heads([sums[1, 0], sums[1, 1]])


def last_kernel(sz, own_ref, back_ref, sinks_ref, dk_ref, dv_ref, out_ref):
    length = sz.length
    totals = [own_ref[0], own_ref[1]]
    sink = sinks_ref[...]
    count = sink.shape[0]
    for tile in range(sz.remote):
        for which in range(2):
            at = slice(which * length, (which + 1) * length)
            totals[which] = totals[which] + back_ref[tile, at].astype(F32)
        rest = jnp.zeros_like(sink)
        for i in range(3):
            pieces = []
            for j in range(sz.slices):
                at = 2 * length + count * (i * sz.slices + j)
                pieces.append(back_ref[tile, at : at + count, :LANES].astype(F32))
            rest = rest + join(pieces, 1)
        sink = sink + rest
    dk_ref[...] = totals[0].astype(BF16)
    dv_ref[...] = totals[1].astype(BF16)
    lane = lax.broadcasted_iota(jnp.int32, sink.shape, 1)
    out_lane = lax.broadcasted_iota(jnp.int32, out_ref.shape, 1)
    line = jnp.zeros(out_ref.shape, F32)
    for pair in range(sz.pairs):
        sums = jnp.sum(jnp.where(lane // BLOCK == pair, sink, 0.0), axis=1, keepdims=True)
        for r in range(count):
            at = (r // 2) * 2 * sz.pairs + 2 * pair + r % 2
            line = jnp.where(out_lane == at, sums[r : r + 1], line)
    out_ref[...] = line


def on_device(ctx_size, queries, keys, values, grad_out, segments, sinks):
    sz = Sizes(queries, keys, ctx_size)
    length, width, remote = sz.length, sz.width, sz.remote
    vmem = pl.BlockSpec(memory_space=pltpu.VMEM)
    hbm = pl.BlockSpec(memory_space=pltpu.HBM)
    shape = jax.ShapeDtypeStruct
    seg_line = segments.reshape(1, length)
    small = remote == 1

    def stay(array):
        return pltpu.with_memory_space_constraint(array, pltpu.HBM)

    def params(mib):
        return pltpu.CompilerParams(vmem_limit_bytes=mib << 20)

    def cost(flops):
        return pl.CostEstimate(flops=flops, bytes_accessed=1 << 20, transcendentals=0)

    tile_flops = 4 * queries.shape[0] * queries.shape[1] * length

    pack_k, pack_v = pl.pallas_call(
        functools.partial(pack_kernel, sz, "ctx"),
        name="pack",
        out_shape=(shape((length + 16, sz.cols), BF16), shape(values.shape, BF16)),
        in_specs=[hbm, hbm, hbm],
        out_specs=(vmem, vmem),
        scratch_shapes=[pltpu.VMEM((1, length), jnp.int32)] + [pltpu.SemaphoreType.DMA] * 3,
        compiler_params=params(4),
    )(stay(keys), stay(values), stay(seg_line))

    def turn(array, shift):
        order = [(i, (i + shift) % ctx_size) for i in range(ctx_size)]
        return lax.ppermute(array, "ctx", order)

    far_k = jnp.stack([turn(pack_k, s) for s in range(1, ctx_size)])
    far_v = jnp.stack([turn(pack_v, s) for s in range(1, ctx_size)])

    stacked = shape((sz.kv_heads, sz.blocks, width, LANES), BF16)
    tiles = shape((sz.kv_heads, sz.near, width), F32)
    stats = shape((sz.stats, width), F32)
    q_here, k_here, g_here, weights, dprob, tops, mass, feats, sink_in = pl.pallas_call(
        functools.partial(near_kernel, sz),
        name="near",
        out_shape=(
            stacked,
            shape(keys.shape, BF16),
            stacked,
            tiles,
            tiles,
            stats,
            stats,
            shape((length, LANES), BF16),
            shape((2 * sz.kv_heads, width), F32),
        ),
        in_specs=[hbm] * 6 + [vmem] * 2,
        out_specs=(vmem,) * 9,
        scratch_shapes=[
            pltpu.VMEM(queries.shape, BF16),
            pltpu.VMEM(grad_out.shape, BF16),
            pltpu.VMEM(values.shape, BF16),
            pltpu.VMEM((1, length), jnp.int32),
            pltpu.SMEM(sinks.shape, F32),
            pltpu.SemaphoreType.DMA((6,)),
        ],
        compiler_params=params(16),
        cost_estimate=cost(2 * tile_flops),
    )(*[stay(a) for a in (queries, keys, values, grad_out, seg_line, sinks)], pack_k, pack_v)

    far_rows = 2 * length if small else 8
    e_far, tops, ratio, inverse, sink_prob = pl.pallas_call(
        functools.partial(stat_kernel, sz, "ctx"),
        name="stat",
        out_shape=(shape((sz.kv_heads, sz.blocks, far_rows, width), F32),) + (stats,) * 4,
        in_specs=[vmem] * 6,
        out_specs=(vmem,) * 5,
        compiler_params=params(16),
        cost_estimate=cost(tile_flops),
    )(q_here, far_k, sink_in, tops, mass, feats)

    many = (8, LANES) if small else (remote, 2 * length, width)
    part, ds_far, delta, sink_rows = pl.pallas_call(
        functools.partial(far_kernel, sz, "ctx"),
        name="far",
        out_shape=(
            shape((remote, sz.tall, sz.cols), BF16),
            shape((sz.kv_heads, sz.blocks, remote, sz.slices, 2 * length, LANES), BF16),
            stats,
            shape((2 * sz.kv_heads, width), F32),
        ),
        in_specs=[vmem] * 12,
        out_specs=(vmem,) * 4,
        scratch_shapes=[
            pltpu.VMEM(many, F32),
            pltpu.VMEM(many, F32),
            pltpu.VMEM((16, LANES) if small else (sz.blocks,) + many, BF16),
        ],
        compiler_params=params(16 if small else 60),
        cost_estimate=cost(3 * tile_flops),
    )(
        q_here, g_here, far_k, far_v, weights, dprob, feats,
        e_far, tops, ratio, inverse, sink_prob,
    )

    back = jnp.stack([turn(part[s - 1], -s) for s in range(1, ctx_size)])

    dq, own = pl.pallas_call(
        functools.partial(grad_kernel, sz, "ctx"),
        name="grad",
        out_shape=(shape(queries.shape, BF16), shape((2,) + keys.shape, F32)),
        in_specs=[vmem] * 9,
        out_specs=(vmem, vmem),
        compiler_params=params(16 if small else 60),
        cost_estimate=cost(4 * tile_flops),
    )(q_here, k_here, g_here, far_k, weights, dprob, ratio, delta, ds_far)

    heads = sinks.shape[0]
    dk, dv, line = pl.pallas_call(
        functools.partial(last_kernel, sz),
        name="last",
        out_shape=(shape(keys.shape, BF16), shape(values.shape, BF16), shape((1, heads), F32)),
        in_specs=[vmem, vmem, vmem],
        out_specs=(vmem, vmem, vmem),
        compiler_params=params(8),
    )(own, back, sink_rows)
    return dq, dk, dv, line.reshape(heads)


def solution(mesh):
    rows = P(("dp", "ctx"), "tp")
    return jax.shard_map(
        functools.partial(on_device, mesh.shape["ctx"]),
        mesh=mesh,
        in_specs=(rows, rows, rows, rows, P(("dp", "ctx")), P("tp")),
        out_specs=(rows, rows, rows, P(("dp", "tp"))),
        check_vma=False,
    )
```
